32 devices in a mesh: gx: 4 (over z), gy: 4 (over y, x), gz: 2 (over core).
Axes of the slice: x: 2, y: 2, z: 4, core: 2. Of those that a mesh axis runs over, the one named last changes fastest.
Arguments:
- panel: float32 [8192, 4096], P(('gx', 'gy', 'gz'))
- treat_start: int32 [8192], P(('gx', 'gy', 'gz')), may hold values from 1024 to 4096
- loading_init: float32 [64, 8192], P(None, ('gx', 'gy', 'gz'))
- factor_init: float32 [64, 4096], P(None, ('gx', 'gy', 'gz'))
- unit_init: float32 [8192], P(('gx', 'gy', 'gz'))
- day_init: float32 [4096], replicated
Outputs:
- loading_out: float32 [64, 8192], P(None, ('gx', 'gy', 'gz'))
- factor_out: float32 [64, 4096], P(None, ('gx', 'gy', 'gz'))
- unit_out: float32 [8192], P(('gx', 'gy', 'gz'))
- day_out: float32 [4096], replicated
The draws below stay inside these ranges and needn't reach their ends.
Inputs may be any that keep to these rules, and one draw needn't show every extreme that they name: A unit is treated from day treat_start on; 4096 means never treated.
All inputs are finite; a program needn't handle non-finite values.
Results may differ from the reference program's by a relative error of at most 0.0001.
Values sent between devices are 32-bit elements; how exact they have to be, the bound alone decides.
A program may use at most 64 MiB of HBM per device.

```python
import jax
import jax.numpy as jnp
from jax import lax

RANK = 64
DAYS = 4096
SWEEPS = 2
UNITS = 8192


def truth_parts(key):
    keys = jax.random.split(jax.random.fold_in(key, 7), 4)
    loading_true = jax.random.normal(keys[0], (UNITS, RANK), jnp.float32)
    factor_true = jax.random.normal(keys[1], (RANK, DAYS), jnp.float32) * RANK ** (-0.5)
    unit_true = jax.random.normal(keys[2], (UNITS,), jnp.float32)
    day_true = 0.5 * jax.random.normal(keys[3], (DAYS,), jnp.float32)
    return (loading_true, factor_true, unit_true, day_true)


def draw_panel(key, part):
    loading_true, factor_true, unit_true, day_true = truth_parts(key)
    keys = jax.random.split(jax.random.fold_in(key, 11), 2)
    rising = 1.0 + 2.0 * jnp.arange(UNITS, dtype=jnp.float32) / max(UNITS - 1, 1)
    spread = jnp.exp(jax.random.uniform(keys[0], (UNITS,), jnp.float32, -1.15, 1.15))
    scales = 0.3 * rising * spread
    noise = jax.random.normal(keys[1], (UNITS, DAYS), jnp.float32)
    signal = jnp.dot(loading_true, factor_true, precision=lax.Precision.HIGHEST)
    return unit_true[:, None] + day_true[None, :] + signal + scales[:, None] * noise


def draw_loading_init(key, part):
    loading_true = truth_parts(key)[0]
    noise = jax.random.normal(jax.random.fold_in(key, 21), (UNITS, RANK), jnp.float32)
    return (loading_true + 0.5 * noise).T


def draw_factor_init(key, part):
    factor_true = truth_parts(key)[1]
    noise = jax.random.normal(jax.random.fold_in(key, 31), (RANK, DAYS), jnp.float32)
    return factor_true + 0.5 * RANK ** (-0.5) * noise


def draw_unit_init(key, part):
    unit_true = truth_parts(key)[2]
    return unit_true + 0.3 * jax.random.normal(jax.random.fold_in(key, 41), (UNITS,), jnp.float32)


def draw_day_init(key, part):
    day_true = truth_parts(key)[3]
    return day_true + 0.3 * jax.random.normal(jax.random.fold_in(key, 51), (DAYS,), jnp.float32)


def place_ends(result, rng, low, top_value):
    index_at = [jax.random.randint(jax.random.fold_in(rng, axis), (), 0, length) for axis, length in enumerate(result.shape)]
    widest = result.shape.index(max(result.shape))
    next_to = index_at[:widest] + [(index_at[widest] + 1) % result.shape[widest]] + index_at[widest + 1:]
    return result.at[tuple(index_at)].set(low).at[tuple(next_to)].set(top_value)


def setup_inputs(seed: int = 0) -> dict:
    streams_of = jax.random.split(jax.random.key(seed), 7)
    panel = draw_panel(jax.random.fold_in(streams_of[6], 71), 0)
    treat_start = place_ends(jax.random.randint(streams_of[1], (UNITS,), DAYS // 4, DAYS + 1), jax.random.fold_in(streams_of[1], 1), DAYS // 4, DAYS).astype(jnp.int32)
    loading_init = draw_loading_init(jax.random.fold_in(streams_of[6], 71), 0)
    factor_init = draw_factor_init(jax.random.fold_in(streams_of[6], 71), 0)
    unit_init = draw_unit_init(jax.random.fold_in(streams_of[6], 71), 0)
    day_init = draw_day_init(jax.random.fold_in(streams_of[6], 71), 0)
    return {"panel": panel, "treat_start": treat_start, "loading_init": loading_init, "factor_init": factor_init, "unit_init": unit_init, "day_init": day_init}


RIDGE = 1.0

def solve_spd(matrix, right):
    lower = jnp.linalg.cholesky(matrix)
    middle = lax.linalg.triangular_solve(lower, right, left_side=True, lower=True)
    return lax.linalg.triangular_solve(lower, middle, left_side=True, lower=True, transpose_a=True)

def reference(panel, treat_start, loading_init, factor_init, unit_init, day_init):
    loading = loading_init
    factors = factor_init
    unit_eff = unit_init
    day_eff = day_init
    ridge_eye = jnp.eye(RANK, dtype=jnp.float32) * RIDGE
    observed = lax.broadcasted_iota(jnp.int32, (UNITS, DAYS), 1) < treat_start[:, None]
    for sweep_index in range(SWEEPS):
        fitted = lax.dot_general(loading.astype(jnp.float32), factors.astype(jnp.float32), (((0,), (0,)), ((), ())), precision=lax.Precision.HIGHEST, preferred_element_type=jnp.float32)
        imputed = jnp.where(observed, panel, unit_eff[:, None] + day_eff[None, :] + fitted)
        without = imputed - fitted
        day_sums = jnp.sum(without, 0)
        row_sums = jnp.sum(without, 1)
        grand = jnp.sum(day_sums) / (UNITS * DAYS)
        day_eff = day_sums / UNITS - grand
        unit_eff = row_sums / DAYS - grand
        resid = imputed - unit_eff[:, None] - day_eff[None, :]
        unit_gram = jnp.dot(loading, loading.T, precision=lax.Precision.HIGHEST)
        weighted = jnp.dot(loading, resid, precision=lax.Precision.HIGHEST)
        factors = solve_spd(unit_gram + ridge_eye, weighted)
        factor_gram = jnp.dot(factors, factors.T, precision=lax.Precision.HIGHEST)
        projected = lax.dot_general(factors.astype(jnp.float32), resid.astype(jnp.float32), (((1,), (1,)), ((), ())), precision=lax.Precision.HIGHEST, preferred_element_type=jnp.float32)
        loading = solve_spd(factor_gram + ridge_eye, projected)
    return (loading, factors, unit_eff, day_eff)
```

```python
import functools

import jax
import jax.numpy as jnp
from jax import lax
from jax.experimental import pallas as pl
from jax.experimental.pallas import tpu as pltpu
from jax.sharding import PartitionSpec as P

SWEEPS = 2
RIDGE = 1.0
WIDTH = 512
LANES = 128
AXES = ("gx", "gy", "gz")
MESH = pl.DeviceIdType.MESH
VMEM = pl.BlockSpec(memory_space=pltpu.VMEM)
ANY = pl.BlockSpec(memory_space=pl.ANY)
F32 = jnp.float32
BF16 = jnp.bfloat16


def mul(left, right, at):
    return lax.dot_general(left, right, ((at[:1], at[1:]), ((), ())), preferred_element_type=F32)


def halves(value):
    high = value.astype(BF16)
    return high, (value - high.astype(F32)).astype(BF16)


def wide_left(value):
    high, low = halves(value)
    return jnp.concatenate([high, high, low], 1)


def wide_right(value):
    high, low = halves(value)
    return jnp.concatenate([high, low, high], 0)


def quadrants(value, rows, cols):
    top = value[:rows, :cols] + value[:rows, cols:2 * cols]
    return top + (value[rows:, :cols] + value[rows:, cols:2 * cols])


def eye(rank):
    return lax.broadcasted_iota(jnp.int32, (rank, rank), 0) == lax.broadcasted_iota(jnp.int32, (rank, rank), 1)


def with_identity(matrix):
    unit = jnp.where(eye(matrix.shape[0]), 1.0, 0.0)
    return jnp.concatenate([matrix + RIDGE * unit, unit], 1)


def eliminate(work, first, last):
    row_at = lax.broadcasted_iota(jnp.int32, work.shape, 0)
    for k in range(first, last):
        pivot_row = work[k:k + 1, :] * (1.0 / work[k:k + 1, k:k + 1])
        work = jnp.where(row_at == k, pivot_row, work - work[:, k:k + 1] * pivot_row)
    return work


def column(row, rank):
    return jnp.sum(jnp.where(eye(rank), row, 0.0), 1, keepdims=True)


class Links:
    def __init__(self, shape, send, recv):
        self.shape, self.send, self.recv = shape, send, recv
        self.here = {axis: lax.axis_index(axis) for axis in AXES}
        self.index, self.open = 0, []

    def at(self, axis, step):
        return lax.rem(self.here[axis] + step, self.shape[axis])

    def device(self, axis, step):
        place = dict(self.here)
        place[axis] = self.at(axis, step)
        return tuple(place[name] for name in AXES)

    def steps(self, axis):
        return range(1, self.shape[axis])

    def meet(self):
        barrier = pltpu.get_barrier_semaphore()
        count = 0
        for axis in AXES:
            for step in self.steps(axis):
                pl.semaphore_signal(barrier, inc=1, device_id=self.device(axis, step), device_id_type=MESH)
                count += 1
        pl.semaphore_wait(barrier, count)

    def copy(self, source, target, axis, step):
        copy = pltpu.make_async_remote_copy(
            source, target, self.send.at[self.index], self.recv.at[self.index],
            device_id=self.device(axis, step), device_id_type=MESH)
        self.index += 1
        copy.start()
        self.open.append(copy)
        return copy

    def settle(self):
        for copy in self.open:
            copy.wait_send()
        self.open = []


def arrive(copies):
    for copy in copies:
        copy.wait_recv()


class SmallSum:
    order = ("gz", "gy", "gx")

    def __init__(self, links, mine, hold):
        self.links, self.mine, self.hold = links, mine, hold
        self.stage, self.slot, self.moving = 0, 0, []

    def start(self, value):
        axis = self.order[self.stage]
        mine = self.mine.at[self.stage]
        mine[...] = value
        self.value = value
        self.first = self.slot
        self.moving = []
        for step in self.links.steps(axis):
            self.moving.append(self.links.copy(mine, self.hold.at[self.slot], axis, step))
            self.slot += 1

    def finish(self):
        arrive(self.moving)
        value = self.mine[self.stage]
        for slot in range(self.first, self.slot):
            value = value + self.hold[slot]
        self.stage += 1
        return value

    def step(self):
        self.start(self.finish())


def kernel(shape, panel_ref, treat_ref, load_ref, fac_ref, unit_ref, day_ref,
           load_out, fac_out, unit_out, day_out,
           pan, xh, xl, blocks, fh, fl, bd, part, hold_z, hold_y, hold_x, sum_z, sum_y,
           gram_mine, gram_hold, tail_mine, tail_hold, lt, lw, ls, limit, ub, rsum, local, send, recv):
    nx, ny, nz = (shape[axis] for axis in AXES)
    devices = nx * ny * nz
    units, days = panel_ref.shape
    rank, w = fac_ref.shape
    chunk = days // nx
    width = min(WIDTH, chunk)
    per = width // w
    total_units = units * devices
    fold = LANES // rank
    links = Links(shape, send, recv)
    x, y, z = (links.here[axis] for axis in AXES)

    def fetch(at):
        return pltpu.make_async_copy(
            panel_ref.at[:, pl.ds(pl.multiple_of(at * chunk, chunk), chunk)], pan.at[at], local.at[at])

    for c in range(nx):
        fetch(c).start()
    blocks[0, x, y, z, 0:rank, :] = fac_ref[...]
    links.meet()

    def gather(buf, consume):
        own = buf.at[x, y, z]
        xs = [links.copy(own, own, "gx", step) for step in links.steps("gx")]
        ys, zs = [], []

        def spread(i):
            block = buf.at[lax.rem(x + nx - i, nx), y, z]
            ys.append([links.copy(block, block, "gy", step) for step in links.steps("gy")])

        def pair(i):
            arrive(ys[i])
            line = buf.at[lax.rem(x + nx - i, nx), :, z]
            zs.append([links.copy(line, line, "gz", step) for step in links.steps("gz")])

        spread(0)
        for i in range(1, nx):
            arrive(xs[i - 1:i])
            spread(i)
        pair(0)
        for i in range(nx):
            if i + 1 < nx:
                pair(i + 1)
            arrive(zs[i])
            consume(i, lax.rem(x + nx - i, nx))

    def take(buf, at):
        for j in range(ny):
            for k in range(nz):
                c = (j * nz + k) * w
                high, low = halves(buf[at, j, k, 0:rank, :])
                fh[at, :, c:c + w] = high
                fl[at, :, c:c + w] = low

    load = load_ref[...]
    flip = jnp.broadcast_to(unit_ref[...], (LANES, units)).T
    ub[...] = flip
    lane = lax.broadcasted_iota(jnp.int32, (units, LANES), 1).astype(F32)
    limit[...] = jnp.broadcast_to(treat_ref[...].astype(F32), (LANES, units)).T - lane
    for c in range(nx):
        bd[c] = day_ref[:, c * chunk:(c + 1) * chunk]
    row_at = lax.broadcasted_iota(jnp.int32, (8, LANES), 0)
    pad = jnp.zeros((8, LANES - rank), F32)

    def impute(at):
        def tile(t, _):
            start = pl.multiple_of(t * width, width)
            cols = pl.ds(start, width)
            high, low = fh[at, :, cols], fl[at, :, cols]
            fitted = mul(lw[...], jnp.concatenate([high, low, high], 0), (1, 0))
            first = (at * chunk + start).astype(F32)
            day = bd[at, :, cols]
            es, xs = [], []
            for c in range(width // LANES):
                span = slice(c * LANES, (c + 1) * LANES)
                fit = fitted[:, span]
                base = ub[...] + day[:, span]
                miss = pan[at, :, pl.ds(pl.multiple_of(start + c * LANES, LANES), LANES)] - base - fit
                e = jnp.where(limit[...] > first + float(c * LANES), miss, 0.0)
                es.append(e)
                xs.append(e + fit)
            total = es[0]
            for e in es[1:]:
                total = total + e
            rsum[...] += total
            sums = jnp.sum(jnp.concatenate(es, 1), 0, keepdims=True)
            xhigh, xlow = halves(jnp.concatenate(xs, 1))
            xh[at, :, cols] = xhigh
            xl[at, :, cols] = xlow
            both = mul(ls[...], xhigh, (1, 0))
            out = both[:rank] + both[rank:] + mul(ls[0:rank, :], xlow, (1, 0))
            for c in range(per):
                place = t * per + c
                span = slice(c * w, (c + 1) * w)
                spot = (at, lax.rem(place, nz), lax.div(place, nz))
                part[spot + (slice(0, rank),)] = out[:, span]
                part[spot + (slice(rank, rank + 8),)] = jnp.where(row_at[:, :w] == 0, sums[:, span], 0.0)
            return 0

        lax.fori_loop(0, chunk // width, tile, 0)

    for sweep in range(SWEEPS):
        if sweep == 0:
            lt[...] = load.T
        turned = lt[...]
        lw[...] = wide_left(turned)
        high, low = halves(load)
        stack = jnp.concatenate([high, low], 0)
        ls[...] = stack
        gram = quadrants(mul(stack, stack, (1, 1)), rank, rank)
        each = rank // fold
        packed = jnp.concatenate([gram[f * each:(f + 1) * each] for f in range(fold)], 1)
        load_sum = jnp.sum(turned, 0, keepdims=True)
        load_sum = jnp.concatenate([load_sum, jnp.zeros((1, LANES - rank), F32)], 1) if rank < LANES else load_sum
        unit_sum = jnp.sum(ub[:, 0:1], 0, keepdims=True)
        extra = jnp.where(row_at == 0, load_sum, jnp.where(row_at == 1, unit_sum, 0.0))
        grams = SmallSum(links, gram_mine.at[sweep], gram_hold.at[sweep])
        grams.start(jnp.concatenate([packed, extra], 0))
        rsum[...] = jnp.zeros_like(rsum)
        hz, hy, hx = hold_z.at[sweep], hold_y.at[sweep], hold_x.at[sweep]
        pieces = []

        def give(at):
            pieces.append({"at": at, "z": [
                links.copy(part.at[at, links.at("gz", step)], hz.at[step - 1, at], "gz", step)
                for step in links.steps("gz")]})

        def across(n):
            piece = pieces[n]
            at = piece["at"]
            arrive(piece["z"])
            value = part[at, z]
            for slot in range(nz - 1):
                value = value + hz[slot, at]
            sum_z[at] = value
            piece["y"] = [
                links.copy(sum_z.at[at, links.at("gy", step)], hy.at[step - 1, at], "gy", step)
                for step in links.steps("gy")]

        def along(n, offset):
            piece = pieces[n]
            at = piece["at"]
            arrive(piece["y"])
            value = sum_z[at, y]
            for slot in range(ny - 1):
                value = value + hy[slot, at]
            sum_y[at] = value
            piece["x"] = [links.copy(sum_y.at[at], hx.at[offset - 1], "gx", offset)] if offset else []

        offsets = [(nx - i) % nx for i in range(nx)] if sweep == 0 else [(i + 1) % nx for i in range(nx)]

        def chunk_step(n, at):
            if sweep == 0:
                fetch(at).wait()
            impute(at)
            give(at)
            if n >= 1:
                across(n - 1)
            if n >= 2:
                along(n - 2, offsets[n - 2])
            if n < 2:
                grams.step()

        if sweep == 0:
            def begin(i, at):
                take(blocks.at[0], at)
                chunk_step(i, at)

            gather(blocks.at[0], begin)
        else:
            for n in range(nx):
                chunk_step(n, lax.rem(x + offsets[n], nx))

        rows = jnp.sum(rsum[...], 1, keepdims=True)
        weighted_rows = jnp.sum(turned * rows, 0, keepdims=True)
        if rank < LANES:
            weighted_rows = jnp.concatenate([weighted_rows, jnp.zeros((1, LANES - rank), F32)], 1)
        row_total = jnp.sum(rows, 0, keepdims=True)
        tails = SmallSum(links, tail_mine.at[sweep], tail_hold.at[sweep])
        tails.start(jnp.where(row_at == 0, weighted_rows, jnp.where(row_at == 1, row_total, 0.0)))
        gram_all = grams.finish()
        across(nx - 1)
        along(nx - 2, offsets[nx - 2])
        tails.step()
        work = jnp.concatenate([gram_all[0:each, f * rank:(f + 1) * rank] for f in range(fold)], 0)
        work = eliminate(with_identity(work), 0, rank // 2)
        along(nx - 1, offsets[nx - 1])
        tails.step()
        inverse = wide_left(eliminate(work, rank // 2, rank)[:, rank:])
        tail_all = tails.finish()
        for piece in pieces:
            arrive(piece["x"])
        value = sum_y[x]
        for slot in range(nx - 1):
            value = value + hx[slot]
        sum_l = column(gram_all[each:each + 1, 0:rank], rank)
        old_units = gram_all[each + 1:each + 2, 0:1] / total_units
        sum_lr = column(tail_all[0:1, 0:rank], rank)
        mean = tail_all[1:2, 0:1] / (total_units * days)
        old_days = sum(jnp.sum(bd[c], 1, keepdims=True) for c in range(nx)) / days
        moved = value[rank:rank + 1, :] / total_units - (mean + old_days)
        shift = (mean + old_units) - moved
        factors = mul(inverse, wide_right(value[0:rank, :] - sum_lr / days + sum_l * shift), (1, 0))
        own = blocks.at[sweep + 1, x, y, z]
        own[0:rank, :] = factors
        own[rank:rank + 8, :] = jnp.where(row_at[:, :w] == 0, moved, 0.0)
        if sweep == SWEEPS - 1:
            fac_out[...] = factors
        delta = rows / days - (mean + old_units)
        buf = blocks.at[sweep + 1]
        sums = {"square": None, "project": None, "plain": None, "days": None}

        def keep(name, value):
            sums[name] = value if sums[name] is None else sums[name] + value

        def project(i, at):
            take(buf, at)
            both = jnp.concatenate([fh[at], fl[at]], 0)
            keep("square", mul(both, both, (1, 1)))
            keep("project", mul(xh[at], both, (1, 1)) + mul(xl[at], both, (1, 1)))
            for j in range(ny):
                for k in range(nz):
                    c = (j * nz + k) * w
                    change = buf[at, j, k, rank:rank + 1, :]
                    block = buf[at, j, k, 0:rank, :]
                    keep("plain", block)
                    keep("days", block * change)
                    bd[at, :, c:c + w] = bd[at, :, c:c + w] + change

        gather(buf, project)
        work = eliminate(with_identity(quadrants(sums["square"], rank, rank)), 0, rank)
        day_term = jnp.sum(sums["days"], 1, keepdims=True)
        plain = jnp.sum(sums["plain"], 1, keepdims=True)
        day_row = jnp.sum(jnp.where(eye(rank), day_term, 0.0), 0, keepdims=True)
        plain_row = jnp.sum(jnp.where(eye(rank), plain, 0.0), 0, keepdims=True)
        project_all = sums["project"][:, :rank] + sums["project"][:, rank:]
        project_all = project_all - delta * plain_row - day_row
        turned = mul(wide_left(project_all), wide_right(work[:, rank:]), (1, 0))
        lt[...] = turned
        load = turned.T
        ub[...] = ub[...] + delta
        links.settle()

    load_out[...] = load
    unit_out[...] = ub[...].T[0:1, :]
    for c in range(nx):
        day_out[:, c * chunk:(c + 1) * chunk] = bd[c]


def body(shape, panel, treat_start, loading_init, factor_init, unit_init, day_init):
    units, days = panel.shape
    rank, w = factor_init.shape
    nx, ny, nz = (shape[axis] for axis in AXES)
    chunk = days // nx
    high = rank + 8
    each = rank * rank // LANES + 8
    peers = nx + ny + nz - 3
    count = SWEEPS * (2 * peers + nx * (ny + nz - 2) + nx - 1) + (SWEEPS + 1) * (nx - 1 + nx * (ny + nz - 2))
    dma = pltpu.SemaphoreType.DMA

    def array(*sizes):
        return jax.ShapeDtypeStruct(sizes, F32)

    loading, factors, unit_eff, day_eff = pl.pallas_call(
        functools.partial(kernel, shape),
        out_shape=(array(rank, units), array(rank, w), array(1, units), array(1, days)),
        in_specs=[ANY] + [VMEM] * 5,
        out_specs=(VMEM,) * 4,
        scratch_shapes=[
            pltpu.VMEM((nx, units, chunk), F32),
            pltpu.VMEM((nx, units, chunk), BF16),
            pltpu.VMEM((nx, units, chunk), BF16),
            pltpu.VMEM((SWEEPS + 1, nx, ny, nz, high, w), F32),
            pltpu.VMEM((nx, rank, chunk), BF16),
            pltpu.VMEM((nx, rank, chunk), BF16),
            pltpu.VMEM((nx, 1, chunk), F32),
            pltpu.VMEM((nx, nz, ny, high, w), F32),
            pltpu.VMEM((SWEEPS, nz - 1, nx, ny, high, w), F32),
            pltpu.VMEM((SWEEPS, ny - 1, nx, high, w), F32),
            pltpu.VMEM((SWEEPS, nx - 1, high, w), F32),
            pltpu.VMEM((nx, ny, high, w), F32),
            pltpu.VMEM((nx, high, w), F32),
            pltpu.VMEM((SWEEPS, 3, each, LANES), F32),
            pltpu.VMEM((SWEEPS, peers, each, LANES), F32),
            pltpu.VMEM((SWEEPS, 3, 8, LANES), F32),
            pltpu.VMEM((SWEEPS, peers, 8, LANES), F32),
            pltpu.VMEM((units, rank), F32),
            pltpu.VMEM((units, 3 * rank), BF16),
            pltpu.VMEM((2 * rank, units), BF16),
            pltpu.VMEM((units, LANES), F32),
            pltpu.VMEM((units, LANES), F32),
            pltpu.VMEM((units, LANES), F32),
            dma((nx,)),
            dma((count,)),
            dma((count,)),
        ],
        compiler_params=pltpu.CompilerParams(collective_id=0, has_side_effects=True, vmem_limit_bytes=60 * 1024 * 1024),
        name="sweeps",
    )(panel, treat_start[None, :], loading_init, factor_init, unit_init[None, :], day_init[None, :])
    return (loading, factors, unit_eff[0], day_eff[0])


def solution(mesh):
    return jax.shard_map(
        functools.partial(body, dict(mesh.shape)),
        mesh=mesh,
        in_specs=(P(AXES, None), P(AXES), P(None, AXES), P(None, AXES), P(AXES), P()),
        out_specs=(P(None, AXES), P(None, AXES), P(AXES), P()),
        check_vma=False,
    )
```

```python
import functools

import jax
import jax.numpy as jnp
from jax import lax
from jax.experimental import pallas as pl
from jax.experimental.pallas import tpu as pltpu
from jax.sharding import PartitionSpec as P

SWEEPS = 2
RIDGE = 1.0
WIDTH = 512
LANES = 128
AXES = ("gx", "gy", "gz")
MESH = pl.DeviceIdType.MESH
VMEM = pl.BlockSpec(memory_space=pltpu.VMEM)
ANY = pl.BlockSpec(memory_space=pl.ANY)
F32 = jnp.float32
BF16 = jnp.bfloat16


def mul(left, right, at):
    return lax.dot_general(left, right, ((at[:1], at[1:]), ((), ())), preferred_element_type=F32)


def halves(value):
    high = value.astype(BF16)
    return high, (value - high.astype(F32)).astype(BF16)


def wide_left(value):
    high, low = halves(value)
    return jnp.concatenate([high, high, low], 1)


def wide_right(value):
    high, low = halves(value)
    return jnp.concatenate([high, low, high], 0)


def quadrants(value, rows, cols):
    top = value[:rows, :cols] + value[:rows, cols:2 * cols]
    return top + (value[rows:, :cols] + value[rows:, cols:2 * cols])


def eye(rank):
    return lax.broadcasted_iota(jnp.int32, (rank, rank), 0) == lax.broadcasted_iota(jnp.int32, (rank, rank), 1)


def with_identity(matrix):
    unit = jnp.where(eye(matrix.shape[0]), 1.0, 0.0)
    return jnp.concatenate([matrix + RIDGE * unit, unit], 1)


def pair_inverse(a, b, c, d):
    scale = 1.0 / (a * d - b * c)
    return ((d * scale, -(b * scale)), (-(c * scale), a * scale))


def product(left, right):
    return [[left[i][0] * right[0][j] + left[i][1] * right[1][j] for j in range(2)] for i in range(2)]


def quad_inverse(m):
    first = pair_inverse(m[0][0], m[0][1], m[1][0], m[1][1])
    upper = product(first, [m[0][2:], m[1][2:]])
    lower = product([m[2][:2], m[3][:2]], first)
    inner = product([m[2][:2], m[3][:2]], upper)
    last = pair_inverse(*(m[2 + i][2 + j] - inner[i][j] for i in range(2) for j in range(2)))
    right = product(upper, last)
    left = product(last, lower)
    more = product(right, lower)
    return [[first[i][0] + more[i][0], first[i][1] + more[i][1], -right[i][0], -right[i][1]] for i in range(2)] + [
        [-left[i][0], -left[i][1], last[i][0], last[i][1]] for i in range(2)]


def eliminate(work, first, last):
    row_at = lax.broadcasted_iota(jnp.int32, work.shape, 0)
    for k in range(4 * first, 4 * last, 4):
        cols = [jnp.broadcast_to(work[:, k + i:k + i + 1], work.shape) for i in range(4)]
        rows = [work[k + i:k + i + 1] for i in range(4)]
        block = quad_inverse([[cols[j][k + i:k + i + 1] for j in range(4)] for i in range(4)])
        pivots = [(b[0] * rows[0] + b[1] * rows[1]) + (b[2] * rows[2] + b[3] * rows[3]) for b in block]
        work = work - (cols[0] * pivots[0] + cols[1] * pivots[1]) - (cols[2] * pivots[2] + cols[3] * pivots[3])
        for i in range(4):
            work = jnp.where(row_at == k + i, pivots[i], work)
    return work


def column(row, rank):
    return jnp.sum(jnp.where(eye(rank), row, 0.0), 1, keepdims=True)


def nearest(here, count):
    lists = [sorted(range(count), key=lambda at: (abs(at - place), at)) for place in range(count)]
    found = []
    for rank in range(count):
        value = lists[0][rank]
        for place in range(1, count):
            value = jnp.where(here == place, lists[place][rank], value)
        found.append(value)
    return found


class Exchange:
    def __init__(self, links, axis, order, source, target):
        self.links, self.axis, self.target = links, axis, target
        self.base = links.take(links.shape[axis])
        for slot, there in enumerate(order):
            copy = self.copy(source(there), links.here[axis], there, slot)
            copy.start()
            links.open.append(copy)

    def copy(self, source, place, there, slot):
        links = self.links
        return pltpu.make_async_remote_copy(
            source, self.target(place), links.send.at[self.base + slot], links.recv.at[self.base + place],
            device_id=links.device(self.axis, there), device_id_type=MESH)

    def wait(self, *places):
        for place in places:
            self.copy(self.target(place), place, place, 0).wait_recv()


class Links:
    def __init__(self, shape, send, recv):
        self.shape, self.send, self.recv = shape, send, recv
        self.here = {axis: lax.axis_index(axis) for axis in AXES}
        self.others = {
            axis: [lax.rem(self.here[axis] + step, shape[axis]) for step in range(1, shape[axis])] for axis in AXES}
        self.index, self.open = 0, []

    def take(self, count):
        self.index += count
        return self.index - count

    def device(self, axis, there):
        return tuple(there if name == axis else self.here[name] for name in AXES)

    def meet(self):
        barrier = pltpu.get_barrier_semaphore()
        count = 0
        for axis in AXES:
            for there in self.others[axis]:
                pl.semaphore_signal(barrier, inc=1, device_id=self.device(axis, there), device_id_type=MESH)
                count += 1
        pl.semaphore_wait(barrier, count)

    def settle(self):
        for copy in self.open:
            copy.wait_send()
        self.open = []


class SmallSum:
    order = ("gz", "gy", "gx")

    def __init__(self, links, hold, value):
        self.links, self.hold, self.stage, self.slot = links, hold, 0, 0
        self.start(value)

    def start(self, value):
        links, axis, slot = self.links, self.order[self.stage], self.slot
        self.hold[slot + links.here[axis]] = value

        def spot(place):
            return self.hold.at[slot + place]

        self.moving = Exchange(links, axis, links.others[axis], lambda there: spot(links.here[axis]), spot)

    def finish(self):
        axis = self.order[self.stage]
        self.moving.wait(*self.links.others[axis])
        value = self.hold[self.slot]
        for place in range(1, self.links.shape[axis]):
            value = value + self.hold[self.slot + place]
        self.slot += self.links.shape[axis]
        self.stage += 1
        return value

    def step(self):
        self.start(self.finish())


def kernel(shape, panel_ref, treat_ref, load_ref, fac_ref, unit_ref, day_ref,
           load_out, fac_out, unit_out, day_out,
           pan, xh, xl, blocks, fh, fl, bd, part, hold_z, hold_y, hold_x, sum_z, sum_y,
           gram_hold, tail_hold, lt, lw, ls, limit, ub, rsum, local, send, recv):
    nx, ny, nz = (shape[axis] for axis in AXES)
    devices = nx * ny * nz
    units, days = panel_ref.shape
    rank, w = fac_ref.shape
    chunk = days // nx
    width = min(WIDTH, chunk)
    per = width // w
    total_units = units * devices
    fold = LANES // rank
    links = Links(shape, send, recv)
    x, y, z = (links.here[axis] for axis in AXES)

    def fetch(at):
        return pltpu.make_async_copy(
            panel_ref.at[:, pl.ds(pl.multiple_of(at * chunk, chunk), chunk)], pan.at[at], local.at[at])

    for c in range(nx):
        fetch(c).start()
    blocks[0, x, y, z, 0:rank, :] = fac_ref[...]
    links.meet()

    line = nearest(x, nx)

    def gather(buf, rows, consume):
        def spot(at, j):
            return buf.at[at, j, z, 0:rows] if rows < buf.shape[3] else buf.at[at, j, z]

        def pair_spot(at):
            return lambda k: buf.at[at, :, k, 0:rows] if rows < buf.shape[3] else buf.at[at, :, k]

        ys, zs = [], []

        def spread(at):
            ys.append(Exchange(links, "gy", links.others["gy"], lambda there: spot(at, y), lambda j: spot(at, j)))

        def pair(n):
            ys[n].wait(*links.others["gy"])
            place = pair_spot(line[n])
            zs.append(Exchange(links, "gz", links.others["gz"], lambda there: place(z), place))

        spread(x)
        xs = Exchange(links, "gx", line[1:], lambda there: spot(x, y), lambda i: spot(i, y))
        for at in line[1:]:
            xs.wait(at)
            spread(at)
        pair(0)
        for n in range(nx):
            if n + 1 < nx:
                pair(n + 1)
            zs[n].wait(*links.others["gz"])
            consume(n, line[n])

    def take(buf, at, shift):
        found = []
        for j in range(ny):
            for k in range(nz):
                c = (j * nz + k) * w
                block = buf[at, j, k, 0:rank, :]
                if shift is not None:
                    block = block + shift
                high, low = halves(block)
                fh[at, :, c:c + w] = high
                fl[at, :, c:c + w] = low
                found.append(block)
        return found

    load = load_ref[...]
    flip = jnp.broadcast_to(unit_ref[...], (LANES, units)).T
    ub[...] = flip
    lane = lax.broadcasted_iota(jnp.int32, (units, LANES), 1).astype(F32)
    limit[...] = jnp.broadcast_to(treat_ref[...].astype(F32), (LANES, units)).T - lane
    for c in range(nx):
        bd[c] = day_ref[:, c * chunk:(c + 1) * chunk]
    row_at = lax.broadcasted_iota(jnp.int32, (8, LANES), 0)
    pad = jnp.zeros((8, LANES - rank), F32)

    def impute(at):
        def tile(t, _):
            start = pl.multiple_of(t * width, width)
            cols = pl.ds(start, width)
            high, low = fh[at, :, cols], fl[at, :, cols]
            fitted = mul(lw[...], jnp.concatenate([high, low, high], 0), (1, 0))
            first = (at * chunk + start).astype(F32)
            day = bd[at, :, cols]
            es, xs = [], []
            for c in range(width // LANES):
                span = slice(c * LANES, (c + 1) * LANES)
                fit = fitted[:, span]
                base = ub[...] + day[:, span]
                miss = pan[at, :, pl.ds(pl.multiple_of(start + c * LANES, LANES), LANES)] - base - fit
                e = jnp.where(limit[...] > first + float(c * LANES), miss, 0.0)
                es.append(e)
                xs.append(e + fit)
            total = es[0]
            for e in es[1:]:
                total = total + e
            rsum[...] += total
            sums = jnp.sum(jnp.concatenate(es, 1), 0, keepdims=True)
            xhigh, xlow = halves(jnp.concatenate(xs, 1))
            xh[at, :, cols] = xhigh
            xl[at, :, cols] = xlow
            both = mul(ls[...], xhigh, (1, 0))
            out = both[:rank] + both[rank:] + mul(ls[0:rank, :], xlow, (1, 0))
            for c in range(per):
                place = t * per + c
                span = slice(c * w, (c + 1) * w)
                spot = (at, lax.rem(place, nz), lax.div(place, nz))
                part[spot + (slice(0, rank),)] = out[:, span]
                part[spot + (slice(rank, rank + 1),)] = sums[:, span]
            return 0

        lax.fori_loop(0, chunk // width, tile, 0)

    for sweep in range(SWEEPS):
        if sweep == 0:
            lt[...] = load.T
        turned = lt[...]
        lw[...] = wide_left(turned)
        high, low = halves(load)
        stack = jnp.concatenate([high, low], 0)
        ls[...] = stack
        gram = quadrants(mul(stack, stack, (1, 1)), rank, rank)
        each = rank // fold
        packed = jnp.concatenate([gram[f * each:(f + 1) * each] for f in range(fold)], 1)
        load_sum = jnp.sum(turned, 0, keepdims=True)
        load_sum = jnp.concatenate([load_sum, jnp.zeros((1, LANES - rank), F32)], 1) if rank < LANES else load_sum
        unit_sum = jnp.sum(ub[:, 0:1], 0, keepdims=True)
        extra = jnp.where(row_at == 0, load_sum, jnp.where(row_at == 1, unit_sum, 0.0))
        grams = SmallSum(links, gram_hold.at[sweep], jnp.concatenate([packed, extra], 0))
        rsum[...] = jnp.zeros_like(rsum)
        hz, hy, hx = hold_z.at[sweep], hold_y.at[sweep], hold_x.at[sweep]
        order = line if sweep == 0 else line[:0:-1] + line[:1]
        by_z, by_y, by_x = [], [], []

        def give(n):
            at = order[n]
            by_z.append(Exchange(
                links, "gz", links.others["gz"], lambda there: part.at[at, there], lambda k: hz.at[k, at]))

        def across(n):
            at = order[n]
            by_z[n].wait(*links.others["gz"])
            value = part[at, z]
            for k in links.others["gz"]:
                value = value + hz[k, at]
            sum_z[at] = value
            by_y.append(Exchange(
                links, "gy", links.others["gy"], lambda there: sum_z.at[at, there], lambda j: hy.at[j, at]))

        def along(n):
            at = order[n]
            by_y[n].wait(*links.others["gy"])
            value = sum_z[at, y]
            for j in links.others["gy"]:
                value = value + hy[j, at]
            sum_y[at] = value

        def forward(n):
            at = order[n]
            copy = pltpu.make_async_remote_copy(
                sum_y.at[at], hx.at[x], send.at[last_base + n], recv.at[last_base + x],
                device_id=links.device("gx", at), device_id_type=MESH)
            copy.start()
            links.open.append(copy)

        last_base = links.take(nx)
        local_piece = 0 if sweep == 0 else nx - 1

        def chunk_step(n):
            if sweep == 0:
                fetch(order[n]).wait()
            impute(order[n])
            give(n)
            if n >= 1:
                across(n - 1)
            if n == 0:
                grams.step()

        if sweep == 0:
            def begin(n, at):
                take(blocks.at[0], at, None)
                chunk_step(n)

            gather(blocks.at[0], rank, begin)
        else:
            for n in range(nx):
                chunk_step(n)

        rows = jnp.sum(rsum[...], 1, keepdims=True)
        weighted_rows = jnp.sum(turned * rows, 0, keepdims=True)
        if rank < LANES:
            weighted_rows = jnp.concatenate([weighted_rows, jnp.zeros((1, LANES - rank), F32)], 1)
        row_total = jnp.sum(rows, 0, keepdims=True)
        tails = SmallSum(
            links, tail_hold.at[sweep], jnp.where(row_at == 0, weighted_rows, jnp.where(row_at == 1, row_total, 0.0)))
        grams.step()
        across(nx - 1)
        tails.step()

        def pass_on(n):
            along(n)
            if n != local_piece:
                forward(n)

        for n in range(nx - 2):
            pass_on(n)
        gram_all = grams.finish()
        work = jnp.concatenate([gram_all[0:each, f * rank:(f + 1) * rank] for f in range(fold)], 0)
        work = eliminate(with_identity(work), 0, rank // 8)
        pass_on(nx - 2)
        tails.step()
        work = eliminate(work, rank // 8, rank // 4)
        pass_on(nx - 1)
        inverse = wide_left(work[:, rank:])
        sum_l = column(gram_all[each:each + 1, 0:rank], rank)
        old_units = gram_all[each + 1:each + 2, 0:1] / total_units
        old_days = sum(jnp.sum(bd[c], 1, keepdims=True) for c in range(nx)) / days
        for at in line[1:]:
            pltpu.make_async_remote_copy(
                hx.at[at], hx.at[at], send.at[last_base], recv.at[last_base + at],
                device_id=links.device("gx", at), device_id_type=MESH).wait_recv()
        value = sum_y[x]
        for at in line[1:]:
            value = value + hx[at]
        moved = value[rank:rank + 1, :] / total_units
        factors = mul(inverse, wide_right(value[0:rank, :] + sum_l * (old_units + old_days - moved)), (1, 0))
        own = blocks.at[sweep + 1, x, y, z]
        own[0:rank, :] = factors
        own[rank:rank + 1, :] = moved - old_days
        buf = blocks.at[sweep + 1]
        sums, after = {}, {}

        def keep(name, value):
            sums[name] = sums[name] + value if name in sums else value

        def project(n, at):
            if n == 0:
                tail_all = tails.finish()
                mean = tail_all[1:2, 0:1] / (total_units * days)
                right = sum_l * (2.0 * mean) - column(tail_all[0:1, 0:rank], rank) / days
                shift = mul(inverse, wide_right(jnp.broadcast_to(right, (rank, LANES))), (1, 0))[:, 0:1]
                after.update(mean=mean, shift=shift, delta=rows / days - (mean + old_units))
            found = take(buf, at, after["shift"])
            both = jnp.concatenate([fh[at], fl[at]], 0)
            keep("square", mul(both, both, (1, 1)))
            keep("project", mul(xh[at], both, (1, 1)) + mul(xl[at], both, (1, 1)))
            for j in range(ny):
                for k in range(nz):
                    c = (j * nz + k) * w
                    change = buf[at, j, k, rank:rank + 1, :] - after["mean"]
                    block = found[j * nz + k]
                    keep("plain", block)
                    keep("days", block * change)
                    bd[at, :, c:c + w] = bd[at, :, c:c + w] + change

        gather(buf, rank + 1, project)
        delta = after["delta"]
        work = eliminate(with_identity(quadrants(sums["square"], rank, rank)), 0, rank // 4)
        day_term = jnp.sum(sums["days"], 1, keepdims=True)
        plain = jnp.sum(sums["plain"], 1, keepdims=True)
        day_row = jnp.sum(jnp.where(eye(rank), day_term, 0.0), 0, keepdims=True)
        plain_row = jnp.sum(jnp.where(eye(rank), plain, 0.0), 0, keepdims=True)
        project_all = sums["project"][:, :rank] + sums["project"][:, rank:]
        project_all = project_all - delta * plain_row - day_row
        turned = mul(wide_left(project_all), wide_right(work[:, rank:]), (1, 0))
        lt[...] = turned
        load = turned.T
        ub[...] = ub[...] + delta
        if sweep == SWEEPS - 1:
            fac_out[...] = factors + after["shift"]
        links.settle()

    load_out[...] = load
    unit_out[...] = ub[...].T[0:1, :]
    for c in range(nx):
        day_out[:, c * chunk:(c + 1) * chunk] = bd[c]


def deliver(*refs):
    for source, target in zip(refs[:4], refs[4:]):
        target[...] = source[...]


def body(shape, panel, treat_start, loading_init, factor_init, unit_init, day_init):
    units, days = panel.shape
    rank, w = factor_init.shape
    nx, ny, nz = (shape[axis] for axis in AXES)
    chunk = days // nx
    high = rank + 1
    each = rank * rank // LANES + 8
    places = nx + ny + nz
    count = SWEEPS * (2 * places + nx * (ny + nz + 1)) + (SWEEPS + 1) * nx * (ny + nz + 1)
    dma = pltpu.SemaphoreType.DMA

    def array(*sizes):
        return jax.ShapeDtypeStruct(sizes, F32)

    outs = (array(rank, units), array(rank, w), array(1, units), array(1, days))
    results = pl.pallas_call(
        functools.partial(kernel, shape),
        out_shape=outs,
        in_specs=[ANY] + [VMEM] * 5,
        out_specs=(VMEM,) * 4,
        scratch_shapes=[
            pltpu.VMEM((nx, units, chunk), F32),
            pltpu.VMEM((nx, units, chunk), BF16),
            pltpu.VMEM((nx, units, chunk), BF16),
            pltpu.VMEM((SWEEPS + 1, nx, ny, nz, high, w), F32),
            pltpu.VMEM((nx, rank, chunk), BF16),
            pltpu.VMEM((nx, rank, chunk), BF16),
            pltpu.VMEM((nx, 1, chunk), F32),
            pltpu.VMEM((nx, nz, ny, high, w), F32),
            pltpu.VMEM((SWEEPS, nz, nx, ny, high, w), F32),
            pltpu.VMEM((SWEEPS, ny, nx, high, w), F32),
            pltpu.VMEM((SWEEPS, nx, high, w), F32),
            pltpu.VMEM((nx, ny, high, w), F32),
            pltpu.VMEM((nx, high, w), F32),
            pltpu.VMEM((SWEEPS, places, each, LANES), F32),
            pltpu.VMEM((SWEEPS, places, 8, LANES), F32),
            pltpu.VMEM((units, rank), F32),
            pltpu.VMEM((units, 3 * rank), BF16),
            pltpu.VMEM((2 * rank, units), BF16),
            pltpu.VMEM((units, LANES), F32),
            pltpu.VMEM((units, LANES), F32),
            pltpu.VMEM((units, LANES), F32),
            dma((nx,)),
            dma((count,)),
            dma((count,)),
        ],
        compiler_params=pltpu.CompilerParams(collective_id=0, has_side_effects=True, vmem_limit_bytes=60 * 1024 * 1024),
        name="sweeps",
    )(panel, treat_start[None, :], loading_init, factor_init, unit_init[None, :], day_init[None, :])
    loading, factors, unit_eff, day_eff = pl.pallas_call(
        deliver, out_shape=outs, in_specs=[VMEM] * 4, out_specs=(VMEM,) * 4, name="deliver")(*results)
    return (loading, factors, unit_eff[0], day_eff[0])


def solution(mesh):
    return jax.shard_map(
        functools.partial(body, dict(mesh.shape)),
        mesh=mesh,
        in_specs=(P(AXES, None), P(AXES), P(None, AXES), P(None, AXES), P(AXES), P()),
        out_specs=(P(None, AXES), P(None, AXES), P(AXES), P()),
        check_vma=False,
    )
```

```python
import functools

import jax
import jax.numpy as jnp
from jax import lax
from jax.experimental import pallas as pl
from jax.experimental.pallas import tpu as pltpu
from jax.sharding import PartitionSpec as P

SWEEPS = 2
RIDGE = 1.0
WIDTH = 512
LANES = 128
AXES = ("gx", "gy", "gz")
MESH = pl.DeviceIdType.MESH
VMEM = pl.BlockSpec(memory_space=pltpu.VMEM)
ANY = pl.BlockSpec(memory_space=pl.ANY)
F32 = jnp.float32
BF16 = jnp.bfloat16


def mul(left, right, at):
    return lax.dot_general(left, right, ((at[:1], at[1:]), ((), ())), preferred_element_type=F32)


def halves(value):
    high = value.astype(BF16)
    return high, (value - high.astype(F32)).astype(BF16)


def wide_left(value):
    high, low = halves(value)
    return jnp.concatenate([high, high, low], 1)


def wide_right(value):
    high, low = halves(value)
    return jnp.concatenate([high, low, high], 0)


def quadrants(value, rows, cols):
    top = value[:rows, :cols] + value[:rows, cols:2 * cols]
    return top + (value[rows:, :cols] + value[rows:, cols:2 * cols])


def eye(rank):
    return lax.broadcasted_iota(jnp.int32, (rank, rank), 0) == lax.broadcasted_iota(jnp.int32, (rank, rank), 1)


def with_identity(matrix):
    unit = jnp.where(eye(matrix.shape[0]), 1.0, 0.0)
    return jnp.concatenate([matrix + RIDGE * unit, unit], 1)


def pair_inverse(a, b, c, d):
    scale = 1.0 / (a * d - b * c)
    return ((d * scale, -(b * scale)), (-(c * scale), a * scale))


def product(left, right):
    return [[left[i][0] * right[0][j] + left[i][1] * right[1][j] for j in range(2)] for i in range(2)]


def quad_inverse(m):
    first = pair_inverse(m[0][0], m[0][1], m[1][0], m[1][1])
    upper = product(first, [m[0][2:], m[1][2:]])
    lower = product([m[2][:2], m[3][:2]], first)
    inner = product([m[2][:2], m[3][:2]], upper)
    last = pair_inverse(*(m[2 + i][2 + j] - inner[i][j] for i in range(2) for j in range(2)))
    right = product(upper, last)
    left = product(last, lower)
    more = product(right, lower)
    return [[first[i][0] + more[i][0], first[i][1] + more[i][1], -right[i][0], -right[i][1]] for i in range(2)] + [
        [-left[i][0], -left[i][1], last[i][0], last[i][1]] for i in range(2)]


def eliminate(work, first, last):
    rank, span = work.shape
    shape = (8, span)
    row_at = lax.broadcasted_iota(jnp.int32, shape, 0)
    tiles = [work[8 * u:8 * u + 8] for u in range(rank // 8)]
    four = range(4)

    def row(value, at):
        return jnp.broadcast_to(value[at:at + 1], shape)

    def lane(value, at):
        return jnp.broadcast_to(value[:, at:at + 1], shape)

    def combine(factors, values):
        return (factors[0] * values[0] + factors[1] * values[1]) + (factors[2] * values[2] + factors[3] * values[3])

    block = None
    for k in range(4 * first, 4 * last, 4):
        here, at = k // 8, k % 8
        cols = [[lane(tile, k + i) for tile in tiles] for i in four]
        rows = [row(tiles[here], at + i) for i in four]
        if block is None:
            block = [[row(cols[j][here], at + i) for j in four] for i in four]
        inverse = quad_inverse(block)
        if k + 4 < 4 * last:
            there, to = (k + 4) // 8, (k + 4) % 8
            ahead = [[lane(rows[i], k + 4 + c) for i in four] for c in four]
            old = [[lane(row(tiles[there], to + i), k + 4 + c) for c in four] for i in four]
            side = [[row(cols[j][there], to + i) for j in four] for i in four]
            near = [[combine(inverse[j], ahead[c]) for j in four] for c in four]
            block = [[old[i][c] - combine(side[i], near[c]) for c in four] for i in four]
        pivots = [combine(inverse[i], rows) for i in four]
        tiles = [tile - combine([cols[i][u] for i in four], pivots) for u, tile in enumerate(tiles)]
        for i in four:
            tiles[here] = jnp.where(row_at == at + i, pivots[i], tiles[here])
    return jnp.concatenate(tiles, 0)


def column(row, rank):
    return jnp.sum(jnp.where(eye(rank), row, 0.0), 1, keepdims=True)


def ranked(here, count, cost):
    lists = [sorted(range(count), key=lambda at: (cost(place, at), at)) for place in range(count)]
    found = []
    for rank in range(count):
        value = lists[0][rank]
        for place in range(1, count):
            value = jnp.where(here == place, lists[place][rank], value)
        found.append(value)
    return found


def apart(left, right):
    return abs(left - right)


def bits_alike(left, right):
    return -bin(left ^ right).count("1")


class Exchange:
    def __init__(self, links, axis, order, source, target):
        self.links, self.axis, self.target = links, axis, target
        self.base = links.take(links.shape[axis])
        for slot, there in enumerate(order):
            copy = self.copy(source(there), links.here[axis], there, slot)
            copy.start()
            links.open.append(copy)

    def copy(self, source, place, there, slot):
        links = self.links
        return pltpu.make_async_remote_copy(
            source, self.target(place), links.send.at[self.base + slot], links.recv.at[self.base + place],
            device_id=links.device(self.axis, there), device_id_type=MESH)

    def wait(self, *places):
        for place in places:
            self.copy(self.target(place), place, place, 0).wait_recv()


class Links:
    def __init__(self, shape, send, recv):
        self.shape, self.send, self.recv = shape, send, recv
        self.here = {axis: lax.axis_index(axis) for axis in AXES}
        self.others = {
            axis: [lax.rem(self.here[axis] + step, shape[axis]) for step in range(1, shape[axis])] for axis in AXES}
        self.others["gy"] = ranked(self.here["gy"], shape["gy"], bits_alike)[:-1]
        self.index, self.open = 0, []

    def take(self, count):
        self.index += count
        return self.index - count

    def device(self, axis, there):
        return tuple(there if name == axis else self.here[name] for name in AXES)

    def greet(self):
        barrier = pltpu.get_barrier_semaphore()
        for axis in AXES:
            for there in self.others[axis]:
                pl.semaphore_signal(barrier, inc=1, device_id=self.device(axis, there), device_id_type=MESH)

    def meet(self):
        pl.semaphore_wait(pltpu.get_barrier_semaphore(), sum(len(self.others[axis]) for axis in AXES))

    def settle(self):
        for copy in self.open:
            copy.wait_send()
        self.open = []


class SmallSum:
    order = ("gz", "gy", "gx")

    def __init__(self, links, hold, value):
        self.links, self.hold, self.stage, self.slot = links, hold, 0, 0
        self.start(value)

    def start(self, value):
        links, axis, slot = self.links, self.order[self.stage], self.slot
        self.hold[slot + links.here[axis]] = value

        def spot(place):
            return self.hold.at[slot + place]

        self.moving = Exchange(links, axis, links.others[axis], lambda there: spot(links.here[axis]), spot)

    def finish(self):
        axis = self.order[self.stage]
        self.moving.wait(*self.links.others[axis])
        value = self.hold[self.slot]
        for place in range(1, self.links.shape[axis]):
            value = value + self.hold[self.slot + place]
        self.slot += self.links.shape[axis]
        self.stage += 1
        return value

    def step(self):
        self.start(self.finish())


def kernel(shape, panel_ref, treat_ref, load_ref, fac_ref, unit_ref, day_ref,
           load_out, fac_out, unit_out, day_out,
           pan, xh, xl, blocks, fh, fl, bd, part, hold_z, hold_y, hold_x, sum_z, sum_y,
           gram_hold, tail_hold, ld, tr, ur, dr, wide, lt, lw, ls, limit, ub, rsum, local, small, send, recv):
    nx, ny, nz = (shape[axis] for axis in AXES)
    devices = nx * ny * nz
    units, days = panel_ref.shape
    rank, w = fac_ref.shape
    chunk = days // nx
    width = min(WIDTH, chunk)
    per = width // w
    total_units = units * devices
    fold = LANES // rank
    links = Links(shape, send, recv)
    x, y, z = (links.here[axis] for axis in AXES)

    def fetch(at):
        return pltpu.make_async_copy(
            panel_ref.at[:, pl.ds(pl.multiple_of(at * chunk, chunk), chunk)], pan.at[at], local.at[at])

    links.greet()
    inputs = [
        pltpu.make_async_copy(source, target, small.at[n]) for n, (source, target) in enumerate((
            (load_ref, ld), (fac_ref, blocks.at[0, x, y, z, 0:rank]), (treat_ref, tr), (unit_ref, ur), (day_ref, dr)))]
    for copy in inputs:
        copy.start()
    for c in range(nx):
        fetch(c).start()
    line = ranked(x, nx, apart)

    def gather(buf, rows, consume, meanwhile):
        def spot(at, j):
            return buf.at[at, j, z, 0:rows] if rows < buf.shape[3] else buf.at[at, j, z]

        def pair_spot(at):
            return lambda k: buf.at[at, :, k, 0:rows] if rows < buf.shape[3] else buf.at[at, :, k]

        ys, zs = [], []

        def spread(at):
            ys.append(Exchange(links, "gy", links.others["gy"], lambda there: spot(at, y), lambda j: spot(at, j)))

        def pair(n):
            ys[n].wait(*links.others["gy"])
            place = pair_spot(line[n])
            zs.append(Exchange(links, "gz", links.others["gz"], lambda there: place(z), place))

        xs = Exchange(links, "gx", line[1:], lambda there: spot(x, y), lambda i: spot(i, y))
        spread(x)
        for n, at in enumerate(line[1:]):
            meanwhile(n)
            xs.wait(at)
            spread(at)
        meanwhile(nx - 1)
        pair(0)
        for n in range(nx):
            if n + 1 < nx:
                pair(n + 1)
            zs[n].wait(*links.others["gz"])
            consume(n, line[n])

    def collect(buf, at, rows):
        parts = [buf[at, j, k, 0:rows, :] for j in range(ny) for k in range(nz)]
        if w % LANES == 0:
            return jnp.concatenate(parts, 1)
        for c, part_value in enumerate(parts):
            wide[0:rows, c * w:(c + 1) * w] = part_value
        return wide[0:rows, :]

    def take(at, value):
        high, low = halves(value)
        fh[at] = high
        fl[at] = low

    each = rank // fold

    def prepare(load, turned):
        lt[...] = turned
        lw[...] = wide_left(turned)
        high, low = halves(load)
        stack = jnp.concatenate([high, low], 0)
        ls[...] = stack
        gram = quadrants(mul(stack, stack, (1, 1)), rank, rank)
        packed = jnp.concatenate([gram[f * each:(f + 1) * each] for f in range(fold)], 1)
        return packed, jnp.sum(turned, 0, keepdims=True)

    def lanes(row):
        return jnp.concatenate([row, jnp.zeros((1, LANES - rank), F32)], 1) if rank < LANES else row

    inputs[0].wait()
    message = prepare(ld[...], ld[...].T)
    inputs[2].wait()
    inputs[3].wait()
    inputs[4].wait()
    ub[...] = jnp.broadcast_to(ur[...], (LANES, units)).T
    lane = lax.broadcasted_iota(jnp.int32, (units, LANES), 1).astype(F32)
    limit[...] = jnp.broadcast_to(tr[...].astype(F32), (LANES, units)).T - lane
    for c in range(nx):
        bd[c] = dr[:, c * chunk:(c + 1) * chunk]
    row_at = lax.broadcasted_iota(jnp.int32, (8, LANES), 0)

    def impute(at):
        def tile(t, _):
            start = pl.multiple_of(t * width, width)
            cols = pl.ds(start, width)
            high, low = fh[at, :, cols], fl[at, :, cols]
            fitted = mul(lw[...], jnp.concatenate([high, low, high], 0), (1, 0))
            first = (at * chunk + start).astype(F32)
            day = bd[at, :, cols]
            es, xs = [], []
            for c in range(width // LANES):
                span = slice(c * LANES, (c + 1) * LANES)
                fit = fitted[:, span]
                base = ub[...] + day[:, span]
                miss = pan[at, :, pl.ds(pl.multiple_of(start + c * LANES, LANES), LANES)] - base - fit
                e = jnp.where(limit[...] > first + float(c * LANES), miss, 0.0)
                es.append(e)
                xs.append(e + fit)
            total = es[0]
            for e in es[1:]:
                total = total + e
            rsum[...] += total
            sums = jnp.sum(jnp.concatenate(es, 1), 0, keepdims=True)
            xhigh, xlow = halves(jnp.concatenate(xs, 1))
            xh[at, :, cols] = xhigh
            xl[at, :, cols] = xlow
            both = mul(ls[...], xhigh, (1, 0))
            out = both[:rank] + both[rank:] + mul(ls[0:rank, :], xlow, (1, 0))
            for c in range(per):
                place = t * per + c
                span = slice(c * w, (c + 1) * w)
                spot = (at, lax.rem(place, nz), lax.div(place, nz))
                part[spot + (slice(0, rank),)] = out[:, span]
                part[spot + (slice(rank, rank + 1),)] = sums[:, span]
            return 0

        lax.fori_loop(0, chunk // width, tile, 0)

    for sweep in range(SWEEPS):
        packed, load_sum = message
        unit_sum = jnp.sum(ub[:, 0:1], 0, keepdims=True)
        extra = jnp.where(row_at == 0, lanes(load_sum), jnp.where(row_at == 1, unit_sum, 0.0))
        grams = []

        def add_grams(n=0):
            if n == 0:
                grams.append(SmallSum(links, gram_hold.at[sweep], jnp.concatenate([packed, extra], 0)))

        rsum[...] = jnp.zeros_like(rsum)
        hz, hy, hx = hold_z.at[sweep], hold_y.at[sweep], hold_x.at[sweep]
        order = line if sweep == 0 else line[:0:-1] + line[:1]
        by_z, by_y, by_x = [], [], []

        def give(n):
            at = order[n]
            by_z.append(Exchange(
                links, "gz", links.others["gz"], lambda there: part.at[at, there], lambda k: hz.at[k, at]))

        def across(n):
            at = order[n]
            by_z[n].wait(*links.others["gz"])
            value = part[at, z]
            for k in links.others["gz"]:
                value = value + hz[k, at]
            sum_z[at] = value
            by_y.append(Exchange(
                links, "gy", links.others["gy"], lambda there: sum_z.at[at, there], lambda j: hy.at[j, at]))

        def along(n):
            at = order[n]
            by_y[n].wait(*links.others["gy"])
            value = sum_z[at, y]
            for j in links.others["gy"]:
                value = value + hy[j, at]
            sum_y[at] = value

        def forward(n):
            at = order[n]
            copy = pltpu.make_async_remote_copy(
                sum_y.at[at], hx.at[x], send.at[last_base + n], recv.at[last_base + x],
                device_id=links.device("gx", at), device_id_type=MESH)
            copy.start()
            links.open.append(copy)

        last_base = links.take(nx)
        local_piece = 0 if sweep == 0 else nx - 1

        def chunk_step(n):
            if sweep == 0:
                fetch(order[n]).wait()
            impute(order[n])
            give(n)
            if n >= 1:
                across(n - 1)
            if n == 0:
                grams[0].step()

        if sweep == 0:
            def begin(n, at):
                take(at, collect(blocks.at[0], at, rank))
                chunk_step(n)

            links.meet()
            inputs[1].wait()
            gather(blocks.at[0], rank, begin, add_grams)
        else:
            add_grams()
            for n in range(nx):
                chunk_step(n)

        rows = jnp.sum(rsum[...], 1, keepdims=True)
        weighted_rows = lanes(jnp.sum(lt[...] * rows, 0, keepdims=True))
        row_total = jnp.sum(rows, 0, keepdims=True)
        tails = SmallSum(
            links, tail_hold.at[sweep], jnp.where(row_at == 0, weighted_rows, jnp.where(row_at == 1, row_total, 0.0)))
        grams[0].step()
        across(nx - 1)
        tails.step()
        for n in range(nx):
            along(n)
            if n != local_piece:
                forward(n)
        tails.step()
        for at in line[1:]:
            pltpu.make_async_remote_copy(
                hx.at[at], hx.at[at], send.at[last_base], recv.at[last_base + at],
                device_id=links.device("gx", at), device_id_type=MESH).wait_recv()
        value = sum_y[x]
        for at in line[1:]:
            value = value + hx[at]
        buf = blocks.at[sweep + 1]
        buf[x, y, z] = value
        held, sums = {}, {}

        def solve_grams(n):
            if n == 0:
                gram_all = grams[0].finish()
                work = jnp.concatenate([gram_all[0:each, f * rank:(f + 1) * rank] for f in range(fold)], 0)
                held["work"] = with_identity(work)
                held["load"] = column(gram_all[each:each + 1, 0:rank], rank)
                held["units"] = gram_all[each + 1:each + 2, 0:1] / total_units
                held["days"] = sum(jnp.sum(bd[c], 1, keepdims=True) for c in range(nx)) / days
            quads = rank // 4
            cuts = [0, quads // 2] + [quads - quads // 2 + quads // 2 * i // (nx - 1) for i in range(1, nx)]
            held["work"] = eliminate(held["work"], cuts[n], cuts[n + 1])
            if n == nx - 1:
                held["inverse"] = wide_left(held["work"][:, rank:])

        def keep(name, value):
            sums[name] = sums[name] + value if name in sums else value

        def solve(sums_at):
            day_sums = sums_at[rank:rank + 1, :] / total_units
            right = sums_at[0:rank, :] + held["load"] * (held["level"] - day_sums) - held["rows"]
            return mul(held["inverse"], wide_right(right), (1, 0)), day_sums - (held["days"] + held["mean"])

        def project(n, at):
            if n == 0:
                tail_all = tails.finish()
                held["mean"] = tail_all[1:2, 0:1] / (total_units * days)
                held["rows"] = column(tail_all[0:1, 0:rank], rank) / days
                held["level"] = held["units"] + held["days"] + 2.0 * held["mean"]
                held["delta"] = rows / days - (held["mean"] + held["units"])
                if sweep == SWEEPS - 1:
                    fac_out[...] = solve(buf[x, y, z])[0]
            factors, change = solve(collect(buf, at, rank + 1))
            take(at, factors)
            both = jnp.concatenate([fh[at], fl[at]], 0)
            keep("square", mul(both, both, (1, 1)))
            keep("project", mul(xh[at], both, (1, 1)) + mul(xl[at], both, (1, 1)))
            moved = factors * change
            for c in range(chunk // LANES):
                keep("plain", factors[:, c * LANES:(c + 1) * LANES])
                keep("days", moved[:, c * LANES:(c + 1) * LANES])
            bd[at] = bd[at] + change

        gather(buf, rank + 1, project, solve_grams)
        delta = held["delta"]
        work = eliminate(with_identity(quadrants(sums["square"], rank, rank)), 0, rank // 4)
        day_term = jnp.sum(sums["days"], 1, keepdims=True)
        plain = jnp.sum(sums["plain"], 1, keepdims=True)
        day_row = jnp.sum(jnp.where(eye(rank), day_term, 0.0), 0, keepdims=True)
        plain_row = jnp.sum(jnp.where(eye(rank), plain, 0.0), 0, keepdims=True)
        project_all = sums["project"][:, :rank] + sums["project"][:, rank:]
        project_all = project_all - delta * plain_row - day_row
        turned = mul(wide_left(project_all), wide_right(work[:, rank:]), (1, 0))
        load = turned.T
        ub[...] = ub[...] + delta
        if sweep < SWEEPS - 1:
            message = prepare(load, turned)
        links.settle()

    load_out[...] = load
    unit_out[...] = ub[...].T[0:1, :]
    for c in range(nx):
        day_out[:, c * chunk:(c + 1) * chunk] = bd[c]


def deliver(*refs):
    for source, target in zip(refs[:4], refs[4:]):
        target[...] = source[...]


def body(shape, panel, treat_start, loading_init, factor_init, unit_init, day_init):
    units, days = panel.shape
    rank, w = factor_init.shape
    nx, ny, nz = (shape[axis] for axis in AXES)
    chunk = days // nx
    high = rank + 1
    each = rank * rank // LANES + 8
    places = nx + ny + nz
    count = SWEEPS * (2 * places + nx * (ny + nz + 1)) + (SWEEPS + 1) * nx * (ny + nz + 1)
    dma = pltpu.SemaphoreType.DMA

    def array(*sizes):
        return jax.ShapeDtypeStruct(sizes, F32)

    outs = (array(rank, units), array(rank, w), array(1, units), array(1, days))
    results = pl.pallas_call(
        functools.partial(kernel, shape),
        out_shape=outs,
        in_specs=[ANY] * 6,
        out_specs=(VMEM,) * 4,
        scratch_shapes=[
            pltpu.VMEM((nx, units, chunk), F32),
            pltpu.VMEM((nx, units, chunk), BF16),
            pltpu.VMEM((nx, units, chunk), BF16),
            pltpu.VMEM((SWEEPS + 1, nx, ny, nz, high, w), F32),
            pltpu.VMEM((nx, rank, chunk), BF16),
            pltpu.VMEM((nx, rank, chunk), BF16),
            pltpu.VMEM((nx, 1, chunk), F32),
            pltpu.VMEM((nx, nz, ny, high, w), F32),
            pltpu.VMEM((SWEEPS, nz, nx, ny, high, w), F32),
            pltpu.VMEM((SWEEPS, ny, nx, high, w), F32),
            pltpu.VMEM((SWEEPS, nx, high, w), F32),
            pltpu.VMEM((nx, ny, high, w), F32),
            pltpu.VMEM((nx, high, w), F32),
            pltpu.VMEM((SWEEPS, places, each, LANES), F32),
            pltpu.VMEM((SWEEPS, places, 8, LANES), F32),
            pltpu.VMEM((rank, units), F32),
            pltpu.VMEM((1, units), jnp.int32),
            pltpu.VMEM((1, units), F32),
            pltpu.VMEM((1, days), F32),
            pltpu.VMEM((high, chunk), F32),
            pltpu.VMEM((units, rank), F32),
            pltpu.VMEM((units, 3 * rank), BF16),
            pltpu.VMEM((2 * rank, units), BF16),
            pltpu.VMEM((units, LANES), F32),
            pltpu.VMEM((units, LANES), F32),
            pltpu.VMEM((units, LANES), F32),
            dma((nx,)),
            dma((5,)),
            dma((count,)),
            dma((count,)),
        ],
        compiler_params=pltpu.CompilerParams(collective_id=0, has_side_effects=True, vmem_limit_bytes=60 * 1024 * 1024),
        name="sweeps",
    )(panel, treat_start[None, :], loading_init, factor_init, unit_init[None, :], day_init[None, :])
    loading, factors, unit_eff, day_eff = pl.pallas_call(
        deliver, out_shape=outs, in_specs=[VMEM] * 4, out_specs=(VMEM,) * 4, name="deliver")(*results)
    return (loading, factors, unit_eff[0], day_eff[0])


def solution(mesh):
    return jax.shard_map(
        functools.partial(body, dict(mesh.shape)),
        mesh=mesh,
        in_specs=(P(AXES, None), P(AXES), P(None, AXES), P(None, AXES), P(AXES), P()),
        out_specs=(P(None, AXES), P(None, AXES), P(AXES), P()),
        check_vma=False,
    )
```

```python
import functools

import jax
import jax.numpy as jnp
from jax import lax
from jax.experimental import pallas as pl
from jax.experimental.pallas import tpu as pltpu
from jax.sharding import PartitionSpec as P

SWEEPS = 2
RIDGE = 1.0
WIDTH = 1024
LANES = 128
AXES = ("gx", "gy", "gz")
MESH = pl.DeviceIdType.MESH
VMEM = pl.BlockSpec(memory_space=pltpu.VMEM)
ANY = pl.BlockSpec(memory_space=pl.ANY)
F32 = jnp.float32
BF16 = jnp.bfloat16


def mul(left, right, at):
    return lax.dot_general(left, right, ((at[:1], at[1:]), ((), ())), preferred_element_type=F32)


def halves(value):
    high = value.astype(BF16)
    return high, (value - high.astype(F32)).astype(BF16)


def wide_left(value):
    high, low = halves(value)
    return jnp.concatenate([high, high, low], 1)


def wide_right(value):
    high, low = halves(value)
    return jnp.concatenate([high, low, high], 0)


def quadrants(value, rows, cols):
    top = value[:rows, :cols] + value[:rows, cols:2 * cols]
    return top + (value[rows:, :cols] + value[rows:, cols:2 * cols])


def eye(rank):
    return lax.broadcasted_iota(jnp.int32, (rank, rank), 0) == lax.broadcasted_iota(jnp.int32, (rank, rank), 1)


def with_identity(matrix):
    unit = jnp.where(eye(matrix.shape[0]), 1.0, 0.0)
    return jnp.concatenate([matrix + RIDGE * unit, unit], 1)


def pair_inverse(a, b, c, d):
    scale = 1.0 / (a * d - b * c)
    return ((d * scale, -(b * scale)), (-(c * scale), a * scale))


def product(left, right):
    return [[left[i][0] * right[0][j] + left[i][1] * right[1][j] for j in range(2)] for i in range(2)]


def quad_inverse(m):
    first = pair_inverse(m[0][0], m[0][1], m[1][0], m[1][1])
    upper = product(first, [m[0][2:], m[1][2:]])
    lower = product([m[2][:2], m[3][:2]], first)
    inner = product([m[2][:2], m[3][:2]], upper)
    last = pair_inverse(*(m[2 + i][2 + j] - inner[i][j] for i in range(2) for j in range(2)))
    right = product(upper, last)
    left = product(last, lower)
    more = product(right, lower)
    return [[first[i][0] + more[i][0], first[i][1] + more[i][1], -right[i][0], -right[i][1]] for i in range(2)] + [
        [-left[i][0], -left[i][1], last[i][0], last[i][1]] for i in range(2)]


def eliminate(work, first, last):
    rank, span = work.shape
    shape = (8, span)
    row_at = lax.broadcasted_iota(jnp.int32, shape, 0)
    tiles = [work[8 * u:8 * u + 8] for u in range(rank // 8)]
    four = range(4)

    def row(value, at):
        return jnp.broadcast_to(value[at:at + 1], shape)

    def lane(value, at):
        return jnp.broadcast_to(value[:, at:at + 1], shape)

    def combine(factors, values):
        return (factors[0] * values[0] + factors[1] * values[1]) + (factors[2] * values[2] + factors[3] * values[3])

    block = None
    for k in range(4 * first, 4 * last, 4):
        here, at = k // 8, k % 8
        cols = [[lane(tile, k + i) for tile in tiles] for i in four]
        rows = [row(tiles[here], at + i) for i in four]
        if block is None:
            block = [[row(cols[j][here], at + i) for j in four] for i in four]
        inverse = quad_inverse(block)
        if k + 4 < 4 * last:
            there, to = (k + 4) // 8, (k + 4) % 8
            ahead = [[lane(rows[i], k + 4 + c) for i in four] for c in four]
            old = [[lane(row(tiles[there], to + i), k + 4 + c) for c in four] for i in four]
            side = [[row(cols[j][there], to + i) for j in four] for i in four]
            near = [[combine(inverse[j], ahead[c]) for j in four] for c in four]
            block = [[old[i][c] - combine(side[i], near[c]) for c in four] for i in four]
        pivots = [combine(inverse[i], rows) for i in four]
        tiles = [tile - combine([cols[i][u] for i in four], pivots) for u, tile in enumerate(tiles)]
        for i in four:
            tiles[here] = jnp.where(row_at == at + i, pivots[i], tiles[here])
    return jnp.concatenate(tiles, 0)


def column(row, rank):
    return jnp.sum(jnp.where(eye(rank), row, 0.0), 1, keepdims=True)


def ranked(here, count, cost):
    lists = [sorted(range(count), key=lambda at: (cost(place, at), at)) for place in range(count)]
    found = []
    for rank in range(count):
        value = lists[0][rank]
        for place in range(1, count):
            value = jnp.where(here == place, lists[place][rank], value)
        found.append(value)
    return found


def apart(left, right):
    return abs(left - right)


def bits_alike(left, right):
    return -bin(left ^ right).count("1")


class Exchange:
    def __init__(self, links, axis, order, source, target):
        self.links, self.axis, self.target = links, axis, target
        self.base = links.take(links.shape[axis])
        for slot, there in enumerate(order):
            copy = self.copy(source(there), links.here[axis], there, slot)
            copy.start()
            links.open.append(copy)

    def copy(self, source, place, there, slot):
        links = self.links
        return pltpu.make_async_remote_copy(
            source, self.target(place), links.send.at[self.base + slot], links.recv.at[self.base + place],
            device_id=links.device(self.axis, there), device_id_type=MESH)

    def wait(self, *places):
        for place in places:
            self.copy(self.target(place), place, place, 0).wait_recv()


class Links:
    def __init__(self, shape, send, recv):
        self.shape, self.send, self.recv = shape, send, recv
        self.here = {axis: lax.axis_index(axis) for axis in AXES}
        self.others = {
            axis: [lax.rem(self.here[axis] + step, shape[axis]) for step in range(1, shape[axis])] for axis in AXES}
        self.others["gy"] = ranked(self.here["gy"], shape["gy"], bits_alike)[:-1]
        self.index, self.open = 0, []

    def take(self, count):
        self.index += count
        return self.index - count

    def device(self, axis, there):
        return tuple(there if name == axis else self.here[name] for name in AXES)

    def greet(self):
        barrier = pltpu.get_barrier_semaphore()
        for axis in AXES:
            for there in self.others[axis]:
                pl.semaphore_signal(barrier, inc=1, device_id=self.device(axis, there), device_id_type=MESH)

    def meet(self):
        pl.semaphore_wait(pltpu.get_barrier_semaphore(), sum(len(self.others[axis]) for axis in AXES))

    def settle(self):
        for copy in self.open:
            copy.wait_send()
        self.open = []


class SmallSum:
    order = ("gz", "gy", "gx")

    def __init__(self, links, hold, value):
        self.links, self.hold, self.stage, self.slot = links, hold, 0, 0
        self.start(value)

    def start(self, value):
        links, axis, slot = self.links, self.order[self.stage], self.slot
        self.hold[slot + links.here[axis]] = value

        def spot(place):
            return self.hold.at[slot + place]

        self.moving = Exchange(links, axis, links.others[axis], lambda there: spot(links.here[axis]), spot)

    def finish(self):
        axis = self.order[self.stage]
        self.moving.wait(*self.links.others[axis])
        value = self.hold[self.slot]
        for place in range(1, self.links.shape[axis]):
            value = value + self.hold[self.slot + place]
        self.slot += self.links.shape[axis]
        self.stage += 1
        return value

    def step(self):
        self.start(self.finish())


def kernel(shape, panel_ref, treat_ref, load_ref, fac_ref, unit_ref, day_ref,
           load_out, fac_out, unit_out, day_out,
           pan, xh, xl, blocks, fh, fl, bd, part, hold_z, hold_y, hold_x, sum_z, sum_y,
           gram_hold, tail_hold, ld, tr, ur, dr, wide, lt, lw, ls, limit, ub, rsum, local, small, send, recv):
    nx, ny, nz = (shape[axis] for axis in AXES)
    devices = nx * ny * nz
    units, days = panel_ref.shape
    rank, w = fac_ref.shape
    chunk = days // nx
    width = min(WIDTH, chunk)
    per = width // w
    total_units = units * devices
    fold = LANES // rank
    links = Links(shape, send, recv)
    x, y, z = (links.here[axis] for axis in AXES)

    def fetch(at):
        return pltpu.make_async_copy(
            panel_ref.at[:, pl.ds(pl.multiple_of(at * chunk, chunk), chunk)], pan.at[at], local.at[at])

    links.greet()
    inputs = [
        pltpu.make_async_copy(source, target, small.at[n]) for n, (source, target) in enumerate((
            (load_ref, ld), (fac_ref, blocks.at[0, x, y, z, 0:rank]), (treat_ref, tr), (unit_ref, ur), (day_ref, dr)))]
    for copy in inputs:
        copy.start()
    for c in range(nx):
        fetch(c).start()
    line = ranked(x, nx, apart)

    def gather(buf, rows, consume, meanwhile):
        def spot(at, j):
            return buf.at[at, j, z, 0:rows] if rows < buf.shape[3] else buf.at[at, j, z]

        def pair_spot(at):
            return lambda k: buf.at[at, :, k, 0:rows] if rows < buf.shape[3] else buf.at[at, :, k]

        ys, zs = [], []

        def spread(at):
            ys.append(Exchange(links, "gy", links.others["gy"], lambda there: spot(at, y), lambda j: spot(at, j)))

        def pair(n):
            ys[n].wait(*links.others["gy"])
            place = pair_spot(line[n])
            zs.append(Exchange(links, "gz", links.others["gz"], lambda there: place(z), place))

        xs = Exchange(links, "gx", line[1:], lambda there: spot(x, y), lambda i: spot(i, y))
        spread(x)
        for n, at in enumerate(line[1:]):
            meanwhile(n)
            xs.wait(at)
            spread(at)
        meanwhile(nx - 1)
        pair(0)
        for n in range(nx):
            if n + 1 < nx:
                pair(n + 1)
            zs[n].wait(*links.others["gz"])
            consume(n, line[n])

    def collect(buf, at, rows):
        parts = [buf[at, j, k, 0:rows, :] for j in range(ny) for k in range(nz)]
        if w % LANES == 0:
            return jnp.concatenate(parts, 1)
        for c, part_value in enumerate(parts):
            wide[0:rows, c * w:(c + 1) * w] = part_value
        return wide[0:rows, :]

    def take(at, value):
        high, low = halves(value)
        fh[at] = high
        fl[at] = low

    each = rank // fold

    def prepare(load, turned):
        lt[...] = turned
        lw[...] = wide_left(turned)
        high, low = halves(load)
        stack = jnp.concatenate([high, low], 0)
        ls[...] = stack
        gram = quadrants(mul(stack, stack, (1, 1)), rank, rank)
        packed = jnp.concatenate([gram[f * each:(f + 1) * each] for f in range(fold)], 1)
        return packed, jnp.sum(turned, 0, keepdims=True)

    def lanes(row):
        return jnp.concatenate([row, jnp.zeros((1, LANES - rank), F32)], 1) if rank < LANES else row

    inputs[0].wait()
    message = prepare(ld[...], ld[...].T)
    inputs[2].wait()
    inputs[3].wait()
    inputs[4].wait()
    ub[...] = jnp.broadcast_to(ur[...], (LANES, units)).T
    lane = lax.broadcasted_iota(jnp.int32, (units, LANES), 1).astype(F32)
    limit[...] = jnp.broadcast_to(tr[...].astype(F32), (LANES, units)).T - lane
    for c in range(nx):
        bd[c] = dr[:, c * chunk:(c + 1) * chunk]
    row_at = lax.broadcasted_iota(jnp.int32, (8, LANES), 0)

    def impute(at):
        def tile(t, _):
            start = pl.multiple_of(t * width, width)
            cols = pl.ds(start, width)
            high, low = fh[at, :, cols], fl[at, :, cols]
            fitted = mul(lw[...], jnp.concatenate([high, low, high], 0), (1, 0))
            first = (at * chunk + start).astype(F32)
            day = bd[at, :, cols]
            es, xs = [], []
            for c in range(width // LANES):
                span = slice(c * LANES, (c + 1) * LANES)
                fit = fitted[:, span]
                base = ub[...] + day[:, span]
                miss = pan[at, :, pl.ds(pl.multiple_of(start + c * LANES, LANES), LANES)] - base - fit
                e = jnp.where(limit[...] > first + float(c * LANES), miss, 0.0)
                es.append(e)
                xs.append(e + fit)
            total = es[0]
            for e in es[1:]:
                total = total + e
            rsum[...] += total
            sums = jnp.sum(jnp.concatenate(es, 1), 0, keepdims=True)
            xhigh, xlow = halves(jnp.concatenate(xs, 1))
            xh[at, :, cols] = xhigh
            xl[at, :, cols] = xlow
            both = mul(ls[...], xhigh, (1, 0))
            out = both[:rank] + both[rank:] + mul(ls[0:rank, :], xlow, (1, 0))
            for c in range(per):
                place = t * per + c
                span = slice(c * w, (c + 1) * w)
                spot = (at, lax.rem(place, nz), lax.div(place, nz))
                part[spot + (slice(0, rank),)] = out[:, span]
                part[spot + (slice(rank, rank + 1),)] = sums[:, span]
            return 0

        lax.fori_loop(0, chunk // width, tile, 0)

    for sweep in range(SWEEPS):
        packed, load_sum = message
        unit_sum = jnp.sum(ub[:, 0:1], 0, keepdims=True)
        extra = jnp.where(row_at == 0, lanes(load_sum), jnp.where(row_at == 1, unit_sum, 0.0))
        grams = []

        def add_grams(n=0):
            if n == 0:
                grams.append(SmallSum(links, gram_hold.at[sweep], jnp.concatenate([packed, extra], 0)))

        rsum[...] = jnp.zeros_like(rsum)
        hz, hy, hx = hold_z.at[sweep], hold_y.at[sweep], hold_x.at[sweep]
        order = line if sweep == 0 else line[:0:-1] + line[:1]
        by_z, by_y, by_x = [], [], []

        def give(n):
            at = order[n]
            by_z.append(Exchange(
                links, "gz", links.others["gz"], lambda there: part.at[at, there], lambda k: hz.at[k, at]))

        def across(n):
            at = order[n]
            by_z[n].wait(*links.others["gz"])
            value = part[at, z]
            for k in links.others["gz"]:
                value = value + hz[k, at]
            sum_z[at] = value
            by_y.append(Exchange(
                links, "gy", links.others["gy"], lambda there: sum_z.at[at, there], lambda j: hy.at[j, at]))

        def along(n):
            at = order[n]
            by_y[n].wait(*links.others["gy"])
            value = sum_z[at, y]
            for j in links.others["gy"]:
                value = value + hy[j, at]
            sum_y[at] = value

        def forward(n):
            at = order[n]
            copy = pltpu.make_async_remote_copy(
                sum_y.at[at], hx.at[x], send.at[last_base + n], recv.at[last_base + x],
                device_id=links.device("gx", at), device_id_type=MESH)
            copy.start()
            links.open.append(copy)

        last_base = links.take(nx)
        local_piece = 0 if sweep == 0 else nx - 1

        def chunk_step(n):
            if sweep == 0:
                fetch(order[n]).wait()
            impute(order[n])
            give(n)
            if n >= 1:
                across(n - 1)
            if n == 0:
                grams[0].step()

        if sweep == 0:
            def begin(n, at):
                take(at, collect(blocks.at[0], at, rank))
                chunk_step(n)

            links.meet()
            inputs[1].wait()
            gather(blocks.at[0], rank, begin, add_grams)
        else:
            add_grams()
            for n in range(nx):
                chunk_step(n)

        rows = jnp.sum(rsum[...], 1, keepdims=True)
        weighted_rows = lanes(jnp.sum(lt[...] * rows, 0, keepdims=True))
        row_total = jnp.sum(rows, 0, keepdims=True)
        tails = SmallSum(
            links, tail_hold.at[sweep], jnp.where(row_at == 0, weighted_rows, jnp.where(row_at == 1, row_total, 0.0)))
        grams[0].step()
        across(nx - 1)
        tails.step()
        for n in range(nx):
            along(n)
            if n != local_piece:
                forward(n)
        tails.step()
        for at in line[1:]:
            pltpu.make_async_remote_copy(
                hx.at[at], hx.at[at], send.at[last_base], recv.at[last_base + at],
                device_id=links.device("gx", at), device_id_type=MESH).wait_recv()
        value = sum_y[x]
        for at in line[1:]:
            value = value + hx[at]
        buf = blocks.at[sweep + 1]
        buf[x, y, z] = value
        earlier, links.open = links.open, []
        held, sums = {}, {}

        def solve_grams(n):
            if n == 0:
                gram_all = grams[0].finish()
                work = jnp.concatenate([gram_all[0:each, f * rank:(f + 1) * rank] for f in range(fold)], 0)
                held["work"] = with_identity(work)
                held["load"] = column(gram_all[each:each + 1, 0:rank], rank)
                held["units"] = gram_all[each + 1:each + 2, 0:1] / total_units
                held["days"] = sum(jnp.sum(bd[c], 1, keepdims=True) for c in range(nx)) / days
            quads = rank // 4
            cuts = [0, quads // 2] + [quads - quads // 2 + quads // 2 * i // (nx - 1) for i in range(1, nx)]
            held["work"] = eliminate(held["work"], cuts[n], cuts[n + 1])
            if n == nx - 1:
                held["inverse"] = wide_left(held["work"][:, rank:])
                for copy in earlier:
                    copy.wait_send()

        def keep(name, value):
            sums[name] = sums[name] + value if name in sums else value

        def solve(sums_at):
            day_sums = sums_at[rank:rank + 1, :] / total_units
            right = sums_at[0:rank, :] + held["load"] * (held["level"] - day_sums) - held["rows"]
            return mul(held["inverse"], wide_right(right), (1, 0)), day_sums - (held["days"] + held["mean"])

        def project(n, at):
            if n == 0:
                tail_all = tails.finish()
                held["mean"] = tail_all[1:2, 0:1] / (total_units * days)
                held["rows"] = column(tail_all[0:1, 0:rank], rank) / days
                held["level"] = held["units"] + held["days"] + 2.0 * held["mean"]
                held["delta"] = rows / days - (held["mean"] + held["units"])
                if sweep == SWEEPS - 1:
                    fac_out[...] = solve(buf[x, y, z])[0]
            factors, change = solve(collect(buf, at, rank + 1))
            take(at, factors)
            both = jnp.concatenate([fh[at], fl[at]], 0)
            keep("square", mul(both, both, (1, 1)))
            keep("project", mul(xh[at], both, (1, 1)) + mul(xl[at], both, (1, 1)))
            moved = factors * change
            for c in range(chunk // LANES):
                keep("plain", factors[:, c * LANES:(c + 1) * LANES])
                keep("days", moved[:, c * LANES:(c + 1) * LANES])
            bd[at] = bd[at] + change

        gather(buf, rank + 1, project, solve_grams)
        delta = held["delta"]
        work = eliminate(with_identity(quadrants(sums["square"], rank, rank)), 0, rank // 4)
        day_term = jnp.sum(sums["days"], 1, keepdims=True)
        plain = jnp.sum(sums["plain"], 1, keepdims=True)
        day_row = jnp.sum(jnp.where(eye(rank), day_term, 0.0), 0, keepdims=True)
        plain_row = jnp.sum(jnp.where(eye(rank), plain, 0.0), 0, keepdims=True)
        project_all = sums["project"][:, :rank] + sums["project"][:, rank:]
        project_all = project_all - delta * plain_row - day_row
        turned = mul(wide_left(project_all), wide_right(work[:, rank:]), (1, 0))
        load = turned.T
        ub[...] = ub[...] + delta
        if sweep < SWEEPS - 1:
            message = prepare(load, turned)

    load_out[...] = load
    unit_out[...] = ub[...].T[0:1, :]
    for c in range(nx):
        day_out[:, c * chunk:(c + 1) * chunk] = bd[c]
    links.settle()


def deliver(*refs):
    for source, target in zip(refs[:4], refs[4:]):
        target[...] = source[...]


def body(shape, panel, treat_start, loading_init, factor_init, unit_init, day_init):
    units, days = panel.shape
    rank, w = factor_init.shape
    nx, ny, nz = (shape[axis] for axis in AXES)
    chunk = days // nx
    high = rank + 1
    each = rank * rank // LANES + 8
    places = nx + ny + nz
    count = SWEEPS * (2 * places + nx * (ny + nz + 1)) + (SWEEPS + 1) * nx * (ny + nz + 1)
    dma = pltpu.SemaphoreType.DMA

    def array(*sizes):
        return jax.ShapeDtypeStruct(sizes, F32)

    outs = (array(rank, units), array(rank, w), array(1, units), array(1, days))
    results = pl.pallas_call(
        functools.partial(kernel, shape),
        out_shape=outs,
        in_specs=[ANY] * 6,
        out_specs=(VMEM,) * 4,
        scratch_shapes=[
            pltpu.VMEM((nx, units, chunk), F32),
            pltpu.VMEM((nx, units, chunk), BF16),
            pltpu.VMEM((nx, units, chunk), BF16),
            pltpu.VMEM((SWEEPS + 1, nx, ny, nz, high, w), F32),
            pltpu.VMEM((nx, rank, chunk), BF16),
            pltpu.VMEM((nx, rank, chunk), BF16),
            pltpu.VMEM((nx, 1, chunk), F32),
            pltpu.VMEM((nx, nz, ny, high, w), F32),
            pltpu.VMEM((SWEEPS, nz, nx, ny, high, w), F32),
            pltpu.VMEM((SWEEPS, ny, nx, high, w), F32),
            pltpu.VMEM((SWEEPS, nx, high, w), F32),
            pltpu.VMEM((nx, ny, high, w), F32),
            pltpu.VMEM((nx, high, w), F32),
            pltpu.VMEM((SWEEPS, places, each, LANES), F32),
            pltpu.VMEM((SWEEPS, places, 8, LANES), F32),
            pltpu.VMEM((rank, units), F32),
            pltpu.VMEM((1, units), jnp.int32),
            pltpu.VMEM((1, units), F32),
            pltpu.VMEM((1, days), F32),
            pltpu.VMEM((high, chunk), F32),
            pltpu.VMEM((units, rank), F32),
            pltpu.VMEM((units, 3 * rank), BF16),
            pltpu.VMEM((2 * rank, units), BF16),
            pltpu.VMEM((units, LANES), F32),
            pltpu.VMEM((units, LANES), F32),
            pltpu.VMEM((units, LANES), F32),
            dma((nx,)),
            dma((5,)),
            dma((count,)),
            dma((count,)),
        ],
        compiler_params=pltpu.CompilerParams(collective_id=0, has_side_effects=True, vmem_limit_bytes=60 * 1024 * 1024),
        name="sweeps",
    )(panel, treat_start[None, :], loading_init, factor_init, unit_init[None, :], day_init[None, :])
    loading, factors, unit_eff, day_eff = pl.pallas_call(
        deliver, out_shape=outs, in_specs=[VMEM] * 4, out_specs=(VMEM,) * 4, name="deliver")(*results)
    return (loading, factors, unit_eff[0], day_eff[0])


def solution(mesh):
    return jax.shard_map(
        functools.partial(body, dict(mesh.shape)),
        mesh=mesh,
        in_specs=(P(AXES, None), P(AXES), P(None, AXES), P(None, AXES), P(AXES), P()),
        out_specs=(P(None, AXES), P(None, AXES), P(AXES), P()),
        check_vma=False,
    )
```

```python
import functools

import jax
import jax.numpy as jnp
from jax import lax
from jax.experimental import pallas as pl
from jax.experimental.pallas import tpu as pltpu
from jax.sharding import PartitionSpec as P

SWEEPS = 2
RIDGE = 1.0
WIDTH = 1024
LANES = 128
AXES = ("gx", "gy", "gz")
MESH = pl.DeviceIdType.MESH
VMEM = pl.BlockSpec(memory_space=pltpu.VMEM)
ANY = pl.BlockSpec(memory_space=pl.ANY)
F32 = jnp.float32
BF16 = jnp.bfloat16


def mul(left, right, at):
    return lax.dot_general(left, right, ((at[:1], at[1:]), ((), ())), preferred_element_type=F32)


def halves(value):
    high = value.astype(BF16)
    return high, (value - high.astype(F32)).astype(BF16)


def wide_left(value):
    high, low = halves(value)
    return jnp.concatenate([high, high, low], 1)


def wide_right(value):
    high, low = halves(value)
    return jnp.concatenate([high, low, high], 0)


def quadrants(value, rows, cols):
    top = value[:rows, :cols] + value[:rows, cols:2 * cols]
    return top + (value[rows:, :cols] + value[rows:, cols:2 * cols])


def eye(rank):
    return lax.broadcasted_iota(jnp.int32, (rank, rank), 0) == lax.broadcasted_iota(jnp.int32, (rank, rank), 1)


def with_identity(matrix):
    unit = jnp.where(eye(matrix.shape[0]), 1.0, 0.0)
    return jnp.concatenate([matrix + RIDGE * unit, unit], 1)


def pair_inverse(a, b, c, d):
    scale = 1.0 / (a * d - b * c)
    return ((d * scale, -(b * scale)), (-(c * scale), a * scale))


def product(left, right):
    return [[left[i][0] * right[0][j] + left[i][1] * right[1][j] for j in range(2)] for i in range(2)]


def quad_inverse(m):
    first = pair_inverse(m[0][0], m[0][1], m[1][0], m[1][1])
    upper = product(first, [m[0][2:], m[1][2:]])
    lower = product([m[2][:2], m[3][:2]], first)
    inner = product([m[2][:2], m[3][:2]], upper)
    last = pair_inverse(*(m[2 + i][2 + j] - inner[i][j] for i in range(2) for j in range(2)))
    right = product(upper, last)
    left = product(last, lower)
    more = product(right, lower)
    return [[first[i][0] + more[i][0], first[i][1] + more[i][1], -right[i][0], -right[i][1]] for i in range(2)] + [
        [-left[i][0], -left[i][1], last[i][0], last[i][1]] for i in range(2)]


def eliminate(work, first, last):
    rank, span = work.shape
    shape = (8, span)
    row_at = lax.broadcasted_iota(jnp.int32, shape, 0)
    tiles = [work[8 * u:8 * u + 8] for u in range(rank // 8)]
    four = range(4)

    def row(value, at):
        return jnp.broadcast_to(value[at:at + 1], shape)

    def lane(value, at):
        return jnp.broadcast_to(value[:, at:at + 1], shape)

    def combine(factors, values):
        return (factors[0] * values[0] + factors[1] * values[1]) + (factors[2] * values[2] + factors[3] * values[3])

    block = None
    for k in range(4 * first, 4 * last, 4):
        here, at = k // 8, k % 8
        cols = [[lane(tile, k + i) for tile in tiles] for i in four]
        rows = [row(tiles[here], at + i) for i in four]
        if block is None:
            block = [[row(cols[j][here], at + i) for j in four] for i in four]
        inverse = quad_inverse(block)
        if k + 4 < 4 * last:
            there, to = (k + 4) // 8, (k + 4) % 8
            ahead = [[lane(rows[i], k + 4 + c) for i in four] for c in four]
            old = [[lane(row(tiles[there], to + i), k + 4 + c) for c in four] for i in four]
            side = [[row(cols[j][there], to + i) for j in four] for i in four]
            near = [[combine(inverse[j], ahead[c]) for j in four] for c in four]
            block = [[old[i][c] - combine(side[i], near[c]) for c in four] for i in four]
        pivots = [combine(inverse[i], rows) for i in four]
        tiles = [tile - combine([cols[i][u] for i in four], pivots) for u, tile in enumerate(tiles)]
        for i in four:
            tiles[here] = jnp.where(row_at == at + i, pivots[i], tiles[here])
    return jnp.concatenate(tiles, 0)


def column(row, rank):
    return jnp.sum(jnp.where(eye(rank), row, 0.0), 1, keepdims=True)


def ranked(here, count, cost):
    lists = [sorted(range(count), key=lambda at: (cost(place, at), at)) for place in range(count)]
    found = []
    for rank in range(count):
        value = lists[0][rank]
        for place in range(1, count):
            value = jnp.where(here == place, lists[place][rank], value)
        found.append(value)
    return found


def apart(left, right):
    return abs(left - right)


def bits_alike(left, right):
    return -bin(left ^ right).count("1")


class Exchange:
    def __init__(self, links, axis, order, source, target):
        self.links, self.axis, self.target = links, axis, target
        self.base = links.take(links.shape[axis])
        for slot, there in enumerate(order):
            copy = self.copy(source(there), links.here[axis], there, slot)
            copy.start()
            links.open.append(copy)

    def copy(self, source, place, there, slot):
        links = self.links
        return pltpu.make_async_remote_copy(
            source, self.target(place), links.send.at[self.base + slot], links.recv.at[self.base + place],
            device_id=links.device(self.axis, there), device_id_type=MESH)

    def wait(self, *places):
        for place in places:
            self.copy(self.target(place), place, place, 0).wait_recv()


class Links:
    def __init__(self, shape, send, recv):
        self.shape, self.send, self.recv = shape, send, recv
        self.here = {axis: lax.axis_index(axis) for axis in AXES}
        self.others = {
            axis: [lax.rem(self.here[axis] + step, shape[axis]) for step in range(1, shape[axis])] for axis in AXES}
        self.others["gy"] = ranked(self.here["gy"], shape["gy"], bits_alike)[:-1]
        self.index, self.open = 0, []

    def take(self, count):
        self.index += count
        return self.index - count

    def device(self, axis, there):
        return tuple(there if name == axis else self.here[name] for name in AXES)

    def greet(self):
        barrier = pltpu.get_barrier_semaphore()
        for axis in AXES:
            for there in self.others[axis]:
                pl.semaphore_signal(barrier, inc=1, device_id=self.device(axis, there), device_id_type=MESH)

    def meet(self):
        pl.semaphore_wait(pltpu.get_barrier_semaphore(), sum(len(self.others[axis]) for axis in AXES))

    def settle(self):
        for copy in self.open:
            copy.wait_send()
        self.open = []


class SmallSum:
    order = ("gz", "gy", "gx")

    def __init__(self, links, hold, value):
        self.links, self.hold, self.stage, self.slot = links, hold, 0, 0
        self.start(value)

    def start(self, value):
        links, axis, slot = self.links, self.order[self.stage], self.slot
        self.hold[slot + links.here[axis]] = value

        def spot(place):
            return self.hold.at[slot + place]

        self.moving = Exchange(links, axis, links.others[axis], lambda there: spot(links.here[axis]), spot)

    def finish(self):
        axis = self.order[self.stage]
        self.moving.wait(*self.links.others[axis])
        value = self.hold[self.slot]
        for place in range(1, self.links.shape[axis]):
            value = value + self.hold[self.slot + place]
        self.slot += self.links.shape[axis]
        self.stage += 1
        return value

    def step(self):
        self.start(self.finish())


def kernel(shape, panel_ref, treat_ref, load_ref, fac_ref, unit_ref, day_ref,
           load_out, fac_out, unit_out, day_out,
           pan, xh, xl, blocks, fh, fl, bd, part, hold_z, hold_y, hold_x, sum_z, sum_y,
           gram_hold, tail_hold, ld, tr, ur, dr, wide, lt, lw, ls, limit, ub, rsum, local, small, send, recv):
    nx, ny, nz = (shape[axis] for axis in AXES)
    devices = nx * ny * nz
    units, days = panel_ref.shape
    rank, w = fac_ref.shape
    chunk = days // nx
    width = min(WIDTH, chunk)
    per = width // w
    total_units = units * devices
    fold = LANES // rank
    links = Links(shape, send, recv)
    x, y, z = (links.here[axis] for axis in AXES)

    def fetch(at):
        return pltpu.make_async_copy(
            panel_ref.at[:, pl.ds(pl.multiple_of(at * chunk, chunk), chunk)], pan.at[at], local.at[at])

    links.greet()
    inputs = [
        pltpu.make_async_copy(source, target, small.at[n]) for n, (source, target) in enumerate((
            (load_ref, ld), (fac_ref, blocks.at[0, x, y, z, 0:rank]), (treat_ref, tr), (unit_ref, ur), (day_ref, dr)))]
    for copy in inputs:
        copy.start()
    for c in range(nx):
        fetch(c).start()
    line = ranked(x, nx, apart)

    def gather(buf, rows, consume, meanwhile):
        def spot(at, j):
            return buf.at[at, j, z, 0:rows] if rows < buf.shape[3] else buf.at[at, j, z]

        def pair_spot(at):
            return lambda k: buf.at[at, :, k, 0:rows] if rows < buf.shape[3] else buf.at[at, :, k]

        ys, zs = [], []

        def spread(at):
            ys.append(Exchange(links, "gy", links.others["gy"], lambda there: spot(at, y), lambda j: spot(at, j)))

        def pair(n):
            ys[n].wait(*links.others["gy"])
            place = pair_spot(line[n])
            zs.append(Exchange(links, "gz", links.others["gz"], lambda there: place(z), place))

        xs = Exchange(links, "gx", line[1:], lambda there: spot(x, y), lambda i: spot(i, y))
        spread(x)
        for n, at in enumerate(line[1:]):
            meanwhile(n)
            xs.wait(at)
            spread(at)
        meanwhile(nx - 1)
        pair(0)
        for n in range(nx):
            if n + 1 < nx:
                pair(n + 1)
            zs[n].wait(*links.others["gz"])
            consume(n, line[n])

    def collect(buf, at, rows):
        parts = [buf[at, j, k, 0:rows, :] for j in range(ny) for k in range(nz)]
        if w % LANES == 0:
            return jnp.concatenate(parts, 1)
        for c, part_value in enumerate(parts):
            wide[0:rows, c * w:(c + 1) * w] = part_value
        return wide[0:rows, :]

    def take(at, value):
        high, low = halves(value)
        fh[at] = high
        fl[at] = low

    each = rank // fold

    def prepare(load, turned):
        lt[...] = turned
        lw[...] = wide_left(turned)
        high, low = halves(load)
        stack = jnp.concatenate([high, low], 0)
        ls[...] = stack
        gram = quadrants(mul(stack, stack, (1, 1)), rank, rank)
        packed = jnp.concatenate([gram[f * each:(f + 1) * each] for f in range(fold)], 1)
        return packed, jnp.sum(turned, 0, keepdims=True)

    def lanes(row):
        return jnp.concatenate([row, jnp.zeros((1, LANES - rank), F32)], 1) if rank < LANES else row

    inputs[0].wait()
    message = prepare(ld[...], ld[...].T)
    inputs[2].wait()
    inputs[3].wait()
    inputs[4].wait()
    ub[...] = jnp.broadcast_to(ur[...], (LANES, units)).T
    lane = lax.broadcasted_iota(jnp.int32, (units, LANES), 1).astype(F32)
    limit[...] = jnp.broadcast_to(tr[...].astype(F32), (LANES, units)).T - lane
    for c in range(nx):
        bd[c] = dr[:, c * chunk:(c + 1) * chunk]
    row_at = lax.broadcasted_iota(jnp.int32, (8, LANES), 0)

    def impute(at):
        def tile(t, _):
            start = pl.multiple_of(t * width, width)
            cols = pl.ds(start, width)
            high, low = fh[at, :, cols], fl[at, :, cols]
            fitted = mul(lw[...], jnp.concatenate([high, low, high], 0), (1, 0))
            first = (at * chunk + start).astype(F32)
            day = bd[at, :, cols]
            es, xs = [], []
            for c in range(width // LANES):
                span = slice(c * LANES, (c + 1) * LANES)
                fit = fitted[:, span]
                base = ub[...] + day[:, span]
                miss = pan[at, :, pl.ds(pl.multiple_of(start + c * LANES, LANES), LANES)] - base - fit
                e = jnp.where(limit[...] > first + float(c * LANES), miss, 0.0)
                es.append(e)
                xs.append(e + fit)
            total = es[0]
            for e in es[1:]:
                total = total + e
            rsum[...] += total
            sums = jnp.sum(jnp.concatenate(es, 1), 0, keepdims=True)
            xhigh, xlow = halves(jnp.concatenate(xs, 1))
            xh[at, :, cols] = xhigh
            xl[at, :, cols] = xlow
            both = mul(ls[...], xhigh, (1, 0))
            out = both[:rank] + both[rank:] + mul(ls[0:rank, :], xlow, (1, 0))
            for c in range(per):
                place = t * per + c
                span = slice(c * w, (c + 1) * w)
                spot = (at, lax.rem(place, nz), lax.div(place, nz))
                part[spot + (slice(0, rank),)] = out[:, span]
                part[spot + (slice(rank, rank + 1),)] = sums[:, span]
            return 0

        lax.fori_loop(0, chunk // width, tile, 0)

    for sweep in range(SWEEPS):
        packed, load_sum = message
        unit_sum = jnp.sum(ub[:, 0:1], 0, keepdims=True)
        extra = jnp.where(row_at == 0, lanes(load_sum), jnp.where(row_at == 1, unit_sum, 0.0))
        grams = []

        def add_grams(n=0):
            if n == 0:
                grams.append(SmallSum(links, gram_hold.at[sweep], jnp.concatenate([packed, extra], 0)))

        rsum[...] = jnp.zeros_like(rsum)
        hz, hy, hx = hold_z.at[sweep], hold_y.at[sweep], hold_x.at[sweep]
        order = line if sweep == 0 else line[:0:-1] + line[:1]
        by_z, by_y, by_x = [], [], []

        def give(n):
            at = order[n]
            by_z.append(Exchange(
                links, "gz", links.others["gz"], lambda there: part.at[at, there], lambda k: hz.at[k, at]))

        def across(n):
            at = order[n]
            by_z[n].wait(*links.others["gz"])
            value = part[at, z]
            for k in links.others["gz"]:
                value = value + hz[k, at]
            sum_z[at] = value
            by_y.append(Exchange(
                links, "gy", links.others["gy"], lambda there: sum_z.at[at, there], lambda j: hy.at[j, at]))

        def along(n):
            at = order[n]
            by_y[n].wait(*links.others["gy"])
            value = sum_z[at, y]
            for j in links.others["gy"]:
                value = value + hy[j, at]
            sum_y[at] = value

        def forward(n):
            at = order[n]
            copy = pltpu.make_async_remote_copy(
                sum_y.at[at], hx.at[x], send.at[last_base + n], recv.at[last_base + x],
                device_id=links.device("gx", at), device_id_type=MESH)
            copy.start()
            links.open.append(copy)

        last_base = links.take(nx)
        local_piece = 0 if sweep == 0 else nx - 1

        def chunk_step(n):
            if sweep == 0:
                fetch(order[n]).wait()
            impute(order[n])
            give(n)
            if n >= 1:
                across(n - 1)
            if n == 0:
                grams[0].step()

        if sweep == 0:
            def begin(n, at):
                take(at, collect(blocks.at[0], at, rank))
                chunk_step(n)

            links.meet()
            inputs[1].wait()
            gather(blocks.at[0], rank, begin, add_grams)
        else:
            add_grams()
            for n in range(nx):
                chunk_step(n)

        rows = jnp.sum(rsum[...], 1, keepdims=True)
        weighted_rows = lanes(jnp.sum(lt[...] * rows, 0, keepdims=True))
        row_total = jnp.sum(rows, 0, keepdims=True)
        tails = SmallSum(
            links, tail_hold.at[sweep], jnp.where(row_at == 0, weighted_rows, jnp.where(row_at == 1, row_total, 0.0)))
        grams[0].step()
        across(nx - 1)
        tails.step()
        for n in range(nx):
            along(n)
            if n != local_piece:
                forward(n)
        tails.step()
        for at in line[1:]:
            pltpu.make_async_remote_copy(
                hx.at[at], hx.at[at], send.at[last_base], recv.at[last_base + at],
                device_id=links.device("gx", at), device_id_type=MESH).wait_recv()
        value = sum_y[x]
        for at in line[1:]:
            value = value + hx[at]
        buf = blocks.at[sweep + 1]
        buf[x, y, z] = value
        earlier, links.open = links.open, []
        held, sums = {}, {}

        def solve_grams(n):
            if n == 0:
                gram_all = grams[0].finish()
                work = jnp.concatenate([gram_all[0:each, f * rank:(f + 1) * rank] for f in range(fold)], 0)
                held["work"] = with_identity(work)
                held["load"] = column(gram_all[each:each + 1, 0:rank], rank)
                held["units"] = gram_all[each + 1:each + 2, 0:1] / total_units
                held["days"] = sum(jnp.sum(bd[c], 1, keepdims=True) for c in range(nx)) / days
            quads = rank // 4
            cuts = [0, quads // 2] + [quads - quads // 2 + quads // 2 * i // (nx - 1) for i in range(1, nx)]
            held["work"] = eliminate(held["work"], cuts[n], cuts[n + 1])
            if n == nx - 1:
                held["inverse"] = wide_left(held["work"][:, rank:])
                for copy in earlier:
                    copy.wait_send()

        def keep(name, value):
            sums[name] = sums[name] + value if name in sums else value

        def solve(sums_at):
            day_sums = sums_at[rank:rank + 1, :] / total_units
            right = sums_at[0:rank, :] + held["load"] * (held["level"] - day_sums) - held["rows"]
            return mul(held["inverse"], wide_right(right), (1, 0)), day_sums - (held["days"] + held["mean"])

        def project(n, at):
            if n == 0:
                tail_all = tails.finish()
                held["mean"] = tail_all[1:2, 0:1] / (total_units * days)
                held["rows"] = column(tail_all[0:1, 0:rank], rank) / days
                held["level"] = held["units"] + held["days"] + 2.0 * held["mean"]
                held["delta"] = rows / days - (held["mean"] + held["units"])
                if sweep == SWEEPS - 1:
                    fac_out[...] = solve(buf[x, y, z])[0]
            factors, change = solve(collect(buf, at, rank + 1))
            take(at, factors)
            both = jnp.concatenate([fh[at], fl[at]], 0)
            keep("square", mul(both, both, (1, 1)))
            keep("project", mul(xh[at], both, (1, 1)) + mul(xl[at], both, (1, 1)))
            moved = factors * change
            for c in range(chunk // LANES):
                keep("plain", factors[:, c * LANES:(c + 1) * LANES])
                keep("days", moved[:, c * LANES:(c + 1) * LANES])
            bd[at] = bd[at] + change

        gather(buf, rank + 1, project, solve_grams)
        delta = held["delta"]
        work = eliminate(with_identity(quadrants(sums["square"], rank, rank)), 0, rank // 4)
        day_term = jnp.sum(sums["days"], 1, keepdims=True)
        plain = jnp.sum(sums["plain"], 1, keepdims=True)
        day_row = jnp.sum(jnp.where(eye(rank), day_term, 0.0), 0, keepdims=True)
        plain_row = jnp.sum(jnp.where(eye(rank), plain, 0.0), 0, keepdims=True)
        project_all = sums["project"][:, :rank] + sums["project"][:, rank:]
        project_all = project_all - delta * plain_row - day_row
        left_high, left_low = halves(project_all)
        right_high, right_low = halves(work[:, rank:])
        turned = mul(left_high, right_high, (1, 0)) + (
            mul(left_high, right_low, (1, 0)) + mul(left_low, right_high, (1, 0)))
        load = turned.T
        ub[...] = ub[...] + delta
        if sweep < SWEEPS - 1:
            message = prepare(load, turned)

    load_out[...] = load
    unit_out[...] = ub[...].T[0:1, :]
    for c in range(nx):
        day_out[:, c * chunk:(c + 1) * chunk] = bd[c]
    links.settle()


def deliver(*refs):
    for source, target in zip(refs[:4], refs[4:]):
        target[...] = source[...]


def body(shape, panel, treat_start, loading_init, factor_init, unit_init, day_init):
    units, days = panel.shape
    rank, w = factor_init.shape
    nx, ny, nz = (shape[axis] for axis in AXES)
    chunk = days // nx
    high = rank + 1
    each = rank * rank // LANES + 8
    places = nx + ny + nz
    count = SWEEPS * (2 * places + nx * (ny + nz + 1)) + (SWEEPS + 1) * nx * (ny + nz + 1)
    dma = pltpu.SemaphoreType.DMA

    def array(*sizes):
        return jax.ShapeDtypeStruct(sizes, F32)

    outs = (array(rank, units), array(rank, w), array(1, units), array(1, days))
    results = pl.pallas_call(
        functools.partial(kernel, shape),
        out_shape=outs,
        in_specs=[ANY] * 6,
        out_specs=(VMEM,) * 4,
        scratch_shapes=[
            pltpu.VMEM((nx, units, chunk), F32),
            pltpu.VMEM((nx, units, chunk), BF16),
            pltpu.VMEM((nx, units, chunk), BF16),
            pltpu.VMEM((SWEEPS + 1, nx, ny, nz, high, w), F32),
            pltpu.VMEM((nx, rank, chunk), BF16),
            pltpu.VMEM((nx, rank, chunk), BF16),
            pltpu.VMEM((nx, 1, chunk), F32),
            pltpu.VMEM((nx, nz, ny, high, w), F32),
            pltpu.VMEM((SWEEPS, nz, nx, ny, high, w), F32),
            pltpu.VMEM((SWEEPS, ny, nx, high, w), F32),
            pltpu.VMEM((SWEEPS, nx, high, w), F32),
            pltpu.VMEM((nx, ny, high, w), F32),
            pltpu.VMEM((nx, high, w), F32),
            pltpu.VMEM((SWEEPS, places, each, LANES), F32),
            pltpu.VMEM((SWEEPS, places, 8, LANES), F32),
            pltpu.VMEM((rank, units), F32),
            pltpu.VMEM((1, units), jnp.int32),
            pltpu.VMEM((1, units), F32),
            pltpu.VMEM((1, days), F32),
            pltpu.VMEM((high, chunk), F32),
            pltpu.VMEM((units, rank), F32),
            pltpu.VMEM((units, 3 * rank), BF16),
            pltpu.VMEM((2 * rank, units), BF16),
            pltpu.VMEM((units, LANES), F32),
            pltpu.VMEM((units, LANES), F32),
            pltpu.VMEM((units, LANES), F32),
            dma((nx,)),
            dma((5,)),
            dma((count,)),
            dma((count,)),
        ],
        compiler_params=pltpu.CompilerParams(collective_id=0, has_side_effects=True, vmem_limit_bytes=60 * 1024 * 1024),
        name="sweeps",
    )(panel, treat_start[None, :], loading_init, factor_init, unit_init[None, :], day_init[None, :])
    loading, factors, unit_eff, day_eff = pl.pallas_call(
        deliver, out_shape=outs, in_specs=[VMEM] * 4, out_specs=(VMEM,) * 4, name="deliver")(*results)
    return (loading, factors, unit_eff[0], day_eff[0])


def solution(mesh):
    return jax.shard_map(
        functools.partial(body, dict(mesh.shape)),
        mesh=mesh,
        in_specs=(P(AXES, None), P(AXES), P(None, AXES), P(None, AXES), P(AXES), P()),
        out_specs=(P(None, AXES), P(None, AXES), P(AXES), P()),
        check_vma=False,
    )
```
